32 devices in a mesh: rep: 1, dp: 32 (over x, y, z, core).
Axes of the slice: x: 2, y: 2, z: 4, core: 2. Of those that a mesh axis runs over, the one named last changes fastest.
Arguments:
- x: bfloat16 [32, 2048, 768], P(('rep', 'dp'))
- dy: bfloat16 [32, 2048, 768], P(('rep', 'dp'))
- w_gate: bfloat16 [2, 768, 6144], replicated
- w_up: bfloat16 [2, 768, 6144], replicated
- w_down: bfloat16 [2, 6144, 768], replicated
- m_w_gate: float32 [2, 768, 6144], P(None, 'dp')
- m_w_up: float32 [2, 768, 6144], P(None, 'dp')
- m_w_down: float32 [2, 6144, 768], P(None, 'dp')
- v_w_gate: float32 [2, 768, 6144], P(None, 'dp')
- v_w_up: float32 [2, 768, 6144], P(None, 'dp')
- v_w_down: float32 [2, 6144, 768], P(None, 'dp')
Outputs:
- output 1: bfloat16 [2, 768, 6144], P('rep')
- output 2: bfloat16 [2, 768, 6144], P('rep')
- output 3: bfloat16 [2, 6144, 768], P('rep')
- output 4: float32 [2, 768, 6144], P('rep', 'dp')
- output 5: float32 [2, 768, 6144], P('rep', 'dp')
- output 6: float32 [2, 6144, 768], P('rep', 'dp')
- output 7: float32 [2, 768, 6144], P('rep', 'dp')
- output 8: float32 [2, 768, 6144], P('rep', 'dp')
- output 9: float32 [2, 6144, 768], P('rep', 'dp')
All inputs are finite; a program needn't handle non-finite values.
Results may differ from the reference program's by a relative error of at most 0.022.
Values are sent between devices in bfloat16 or wider.
A program may use at most 2 GiB of HBM per device.

```python
import jax
import jax.numpy as jnp
from jax import lax

SEQUENCES = 32
TOKENS = 2048
D = 768
FF = 6144
LAYERS = 2
NAMES = ("w_gate", "w_up", "w_down")
SHAPES = {"w_gate": (LAYERS, D, FF), "w_up": (LAYERS, D, FF), "w_down": (LAYERS, FF, D)}


def bump(key, n, height):
    away = (jnp.arange(n, dtype=jnp.int32) - jax.random.randint(key, (), 0, n, jnp.int32)) % n
    return jnp.where(away < n // 8, height, 1.0)


def together(key, own, strength):
    shared = jax.random.normal(key, own.shape[1:], jnp.float32)
    return (own + strength * shared) * lax.rsqrt(1 + strength * strength)


def setup_inputs(seed: int = 0, part: int = 0) -> dict:
    kx, kdy, ka, kb, kz, kf, kh, kl, *keys = jax.random.split(jax.random.key(seed), 8 + 3 * len(NAMES))
    kx, kdy, ka, kb = (jax.random.fold_in(k, part) for k in (kx, kdy, ka, kb))
    kw, km, kv = (keys[i::3] for i in range(3))
    shape = (SEQUENCES, TOKENS, D)
    much_x, much_dy = jax.random.uniform(kz, (2,), jnp.float32, 0.0, 1.0)
    loud = 2.0 ** jax.random.uniform(jax.random.fold_in(kz, 1), (), jnp.float32, -1.0, 2.0)
    layers = 2.0 ** jax.random.uniform(kl, (LAYERS, 1, 1), jnp.float32, -1.0, 1.0)
    x = together(ka, jax.random.normal(kx, shape, jnp.float32), much_x) * bump(kf, D, 4.0)
    dy = together(kb, jax.random.normal(kdy, shape, jnp.float32), much_dy)
    drawn = {"x": x.astype(jnp.bfloat16), "dy": (loud * dy * (SEQUENCES * TOKENS) ** -0.5).astype(jnp.bfloat16)}
    for key, name in zip(kw, NAMES, strict=True):
        w = jax.random.normal(key, SHAPES[name], jnp.float32) * SHAPES[name][1] ** -0.5
        drawn[name] = (w * {"w_gate": 1.0, "w_up": bump(kh, FF, 4.0), "w_down": layers}[name]).astype(jnp.bfloat16)
    for key, name in zip(km, NAMES, strict=True):
        drawn[f"m_{name}"] = 0.1 * jax.random.normal(key, SHAPES[name], jnp.float32)
    for key, name in zip(kv, NAMES, strict=True):
        drawn[f"v_{name}"] = jax.random.uniform(key, SHAPES[name], jnp.float32, 0.005, 0.015)
    return drawn


def matmul(a, w):
    return jnp.dot(a, w, preferred_element_type=jnp.float32).astype(jnp.bfloat16)


def normed(h):
    wide = h.astype(jnp.float32)
    scale = lax.rsqrt(jnp.mean(wide**2, -1, keepdims=True) + 1e-6)
    return (wide * scale).astype(jnp.bfloat16)


def layer(h, w):
    a = normed(h)
    gate = jnp.dot(a, w["w_gate"], preferred_element_type=jnp.float32)
    up = jnp.dot(a, w["w_up"], preferred_element_type=jnp.float32)
    return h + matmul((jax.nn.silu(gate) * up).astype(jnp.bfloat16), w["w_down"])


def adamw(w, m, v, g):
    m = 0.9 * m + 0.1 * g
    v = 0.95 * v + 0.05 * g * g
    step = m * lax.rsqrt(v + 1e-8) + 0.1 * w
    return (w - 0.02 * step).astype(jnp.bfloat16), m, v


def stack(weights, h):
    return lax.scan(lambda h, w: (layer(h, w), None), h, weights)[0]


def reference(x, dy, w_gate, w_up, w_down, m_w_gate, m_w_up, m_w_down, v_w_gate, v_w_up, v_w_down):
    weights = dict(zip(NAMES, (w_gate, w_up, w_down), strict=True))

    def take(so_far, sequence):
        h, by_y = sequence
        _, back = jax.vjp(lambda w: stack(w, h), weights)
        return jax.tree.map(lambda total, term: total + term.astype(jnp.float32), so_far, back(by_y)[0]), None

    none_yet = {name: jnp.zeros(w.shape, jnp.float32) for name, w in weights.items()}
    by_weights, _ = lax.scan(take, none_yet, (x, dy))
    gradients = [by_weights[name].astype(jnp.bfloat16).astype(jnp.float32) for name in NAMES]
    new = [
        adamw(w.astype(jnp.float32), m, v, g)
        for w, m, v, g in zip((w_gate, w_up, w_down), (m_w_gate, m_w_up, m_w_down), (v_w_gate, v_w_up, v_w_down), gradients, strict=True)
    ]
    return tuple(one[which] for which in range(3) for one in new)
```

```python
import jax
import jax.numpy as jnp
from jax import lax
from jax.sharding import PartitionSpec as P

BF = jnp.bfloat16
F32 = jnp.float32


def dot(a, b, dims):
    return lax.dot_general(a, b, (dims, ((), ())), preferred_element_type=F32)


def scale_of(h):
    wide = h.astype(F32)
    return wide, lax.rsqrt(jnp.mean(wide**2, -1, keepdims=True) + 1e-6)


def norm_back(h, da):
    wide, scale = scale_of(h)
    da = da.astype(F32)
    along = jnp.sum(da * wide, -1, keepdims=True)
    return (da * scale - wide * (scale**3 * along / h.shape[-1])).astype(BF)


def gated(gate, up):
    return (jax.nn.silu(gate) * up).astype(BF)


def gated_back(gate, up, dp):
    s = jax.nn.sigmoid(gate)
    dp = dp.astype(F32)
    d_up = dp * (gate * s)
    d_gate = dp * up * (s * (1 + gate * (1 - s)))
    return d_gate.astype(BF), d_up.astype(BF)


def adamw(w, m, v, g):
    g = g.astype(F32)
    w = w.astype(F32)
    m = 0.9 * m + 0.1 * g
    v = 0.95 * v + 0.05 * g * g
    step = m * lax.rsqrt(v + 1e-8) + 0.1 * w
    return (w - 0.02 * step).astype(BF), m, v


NN, NT, TN = ((1,), (0,)), ((1,), (1,)), ((0,), (0,))


def solution(mesh):
    axis = "dp"
    n = mesh.shape["dp"]

    def step(x, dy, *arrays):
        wg, wu, wd = arrays[:3]
        ms, vs = arrays[3:6], arrays[6:9]
        x, dy = x[0], dy[0]
        layers = wg.shape[0]
        me = lax.axis_index(axis)
        new = [[None] * layers for _ in range(3)]

        def update(which, layer, grad):
            g = lax.psum_scatter(grad.astype(BF), axis, scatter_dimension=0, tiled=True)
            w = arrays[which][layer]
            rows = w.shape[0] // n
            mine = lax.dynamic_slice_in_dim(w, me * rows, rows, 0)
            w, m, v = adamw(mine, ms[which][layer], vs[which][layer], g)
            w = lax.all_gather(w, axis, axis=0, tiled=True)
            new[which][layer] = (w, m, v)

        h = x
        saved = []
        for layer in range(layers):
            wide, scale = scale_of(h)
            a = (wide * scale).astype(BF)
            gate, up = dot(a, wg[layer], NN), dot(a, wu[layer], NN)
            p = gated(gate, up)
            saved.append((h, a, gate, up, p))
            if layer < layers - 1:
                h = h + dot(p, wd[layer], NN).astype(BF)
        dh = dy
        for layer in reversed(range(layers)):
            h, a, gate, up, p = saved[layer]
            update(2, layer, dot(p, dh, TN))
            dp = dot(dh, wd[layer], NT).astype(BF)
            d_gate, d_up = gated_back(gate, up, dp)
            update(0, layer, dot(a, d_gate, TN))
            update(1, layer, dot(a, d_up, TN))
            if layer:
                da = dot(d_gate, wg[layer], NT).astype(BF) + dot(d_up, wu[layer], NT).astype(BF)
                dh = dh + norm_back(h, da)
        return tuple(jnp.stack([new[i][layer][k] for layer in range(layers)]) for k in range(3) for i in range(3))

    seq = P(("rep", "dp"))
    whole = P()
    rows = P(None, "dp")
    return jax.shard_map(
        step,
        mesh=mesh,
        in_specs=(seq, seq) + (whole,) * 3 + (rows,) * 6,
        out_specs=(P("rep"),) * 3 + (P("rep", "dp"),) * 6,
        check_vma=False,
    )
```

```python
import functools

import jax
import jax.numpy as jnp
from jax import lax
from jax.experimental import pallas as pl
from jax.experimental.pallas import tpu as pltpu
from jax.sharding import PartitionSpec as P

BF = jnp.bfloat16
F32 = jnp.float32
MESH = pl.DeviceIdType.MESH
NN, NT = ((1,), (0,)), ((1,), (1,))

CORE, Z0, Z1, Y, X = 1, 2, 4, 8, 16
ORDERS = ((CORE, X, Z0, Y, Z1), (CORE, Y, Z0, X, Z1))
STAGES = 5
CHUNKS = 6
PARTS = 3
PIECES = 2 * (CHUNKS + PARTS)
FRONT = 4


def dot(a, b, dims=NN):
    return lax.dot_general(a, b, (dims, ((), ())), preferred_element_type=F32)


def bit_of(i, bit):
    return (i // bit) % 2


def place(i, order):
    at = 0
    for bit in order:
        at = at * 2 + bit_of(i, bit)
    return at


def sigmoid(x):
    return 1.0 / (1.0 + jnp.exp(-x))


def normed(h):
    wide = h.astype(F32)
    return (wide * lax.rsqrt(jnp.mean(wide**2, -1, keepdims=True) + 1e-6)).astype(BF)


def adamw(w, m, v, g):
    m = 0.9 * m + 0.1 * g
    v = 0.95 * v + 0.05 * g * g
    step = m * lax.rsqrt(v + 1e-8) + 0.1 * w
    return (w - 0.02 * step).astype(BF), m, v


def forward_kernel(x_ref, wg_ref, wu_ref, wd_ref, p_ref, h_ref, a_all, total):
    chunk, tile = pl.program_id(0), pl.program_id(1)
    rows = p_ref.shape[0]
    here = pl.ds(pl.multiple_of(tile * rows, rows), rows)

    @pl.when(chunk == 0)
    def _():
        a_all[here, :] = normed(x_ref[here, :])

    a = a_all[here, :]
    gate, up = dot(a, wg_ref[...]), dot(a, wu_ref[...])
    p = (gate * sigmoid(gate) * up).astype(BF)
    p_ref[...] = p

    @pl.when(chunk == 0)
    def _():
        total[here, :] = dot(p, wd_ref[...])

    @pl.when(chunk > 0)
    def _():
        total[here, :] += dot(p, wd_ref[...])

    @pl.when(chunk == pl.num_programs(0) - 1)
    def _():
        down = total[here, :].astype(BF).astype(F32)
        h_ref[here, :] = (x_ref[here, :].astype(F32) + down).astype(BF)


def forward(x, wg, wu, wd, layer):
    tokens, d = x.shape
    ff = wg.shape[-1]
    c, rows = ff // CHUNKS, min(512, tokens)
    return pl.pallas_call(
        forward_kernel,
        name="forward",
        grid=(CHUNKS, tokens // rows),
        in_specs=[
            pl.BlockSpec((tokens, d), lambda i, t: (0, 0)),
            pl.BlockSpec((None, d, c), lambda i, t: (layer, 0, i)),
            pl.BlockSpec((None, d, c), lambda i, t: (layer, 0, i)),
            pl.BlockSpec((None, c, d), lambda i, t: (layer, i, 0)),
        ],
        out_specs=[pl.BlockSpec((rows, c), lambda i, t: (t, i)), pl.BlockSpec((tokens, d), lambda i, t: (0, 0))],
        out_shape=[jax.ShapeDtypeStruct((tokens, ff), BF), jax.ShapeDtypeStruct((tokens, d), BF)],
        scratch_shapes=[pltpu.VMEM((tokens, d), BF), pltpu.VMEM((tokens, d), F32)],
        compiler_params=pltpu.CompilerParams(vmem_limit_bytes=60 << 20),
        cost_estimate=pl.CostEstimate(flops=6 * tokens * d * ff, bytes_accessed=60 << 20, transcendentals=0),
    )(x, wg, wu, wd)


def step_kernel(
    x_hbm, dy_hbm, h_hbm, p0_hbm, wg_hbm, wu_hbm, wd_hbm, mg_hbm, mu_hbm, md_hbm, vg_hbm, vu_hbm, vd_hbm,
    wa_out, wb_out, mg_out, mu_out, md_out, vg_out, vu_out, vd_out, p1_hbm,
    a, at, dh, dht, wg, wu, wd, dg, du, ps, da, ga, gb, *rest,
):
    (ra, rb, sa, sb), rest = (rest[0:5], rest[5:10], rest[10:14], rest[14:18]), rest[18:]
    wn, mo, vo, wo, mo_d, vo_d, wo_d, rest = *rest[:7], rest[7:]
    rs_send, rs_recv, ag_send, ag_recv, own_sem, load_sem, w_sem, p_sem, opt_sem = rest

    tokens, d = a.shape
    c = wg.shape[1]
    r = d // 32
    e = d // PARTS
    rows = ps.shape[1]
    tiles = tokens // rows
    wide = 4 * 8 * r
    me = lax.axis_index("dp")
    g_bufs, r_bufs, s_bufs, w_outs = (ga, gb), (ra, rb), (sa, sb), (wa_out, wb_out)
    mine = [place(me, order) for order in ORDERS]

    barrier = pltpu.get_barrier_semaphore()
    for bit in (CORE, Z0, Z1, Y, X):
        other = me + bit * (1 - 2 * bit_of(me, bit))
        pl.semaphore_signal(barrier, inc=1, device_id={"dp": other}, device_id_type=MESH)
    pl.semaphore_wait(barrier, 5)

    def rs_copy(half, stage, parity):
        bit = ORDERS[half][stage]
        own, n = bit_of(me, bit), 16 >> stage
        source = g_bufs[half].at[parity] if stage == 0 else s_bufs[half][stage - 1]
        return pltpu.make_async_remote_copy(
            src_ref=source.at[pl.ds((1 - own) * n, n)],
            dst_ref=r_bufs[half][stage].at[parity],
            send_sem=rs_send.at[half, stage],
            recv_sem=rs_recv.at[half, stage, parity],
            device_id={"dp": me + bit * (1 - 2 * own)},
            device_id_type=MESH,
        )

    def rs_start(stage, piece):
        for half in range(2):
            rs_copy(half, stage, piece % 2).start()

    def rs_finish(stage, piece):
        for half in range(2):
            copy = rs_copy(half, stage, piece % 2)
            copy.wait_send()
            copy.wait_recv()
        for half in range(2):
            own, n = bit_of(me, ORDERS[half][stage]), 16 >> stage
            source = g_bufs[half].at[piece % 2] if stage == 0 else s_bufs[half][stage - 1]
            got, to = r_bufs[half][stage].at[piece % 2], s_bufs[half][stage]

            def add(i, _, source=source, got=got, to=to, own=own, n=n):
                to[i] = (source[own * n + i].astype(F32) + got[i].astype(F32)).astype(BF)
                return 0

            lax.fori_loop(0, n, add, 0)

    def rs_sum(half, piece):
        stage = STAGES - 1
        own = bit_of(me, ORDERS[half][stage])
        total = s_bufs[half][stage - 1][own].astype(F32) + r_bufs[half][stage][piece % 2, 0].astype(F32)
        return total.astype(BF).astype(F32)

    def ag_copy(half, stage, piece):
        bit = ORDERS[half][STAGES - 1 - stage]
        n = 1 << stage
        if stage == 0:
            source, to = wn.at[half], w_outs[half].at[piece, mine[half]]
        else:
            source = to = w_outs[half].at[piece, pl.ds((mine[half] // n) * n, n)]
        return pltpu.make_async_remote_copy(
            src_ref=source,
            dst_ref=to,
            send_sem=ag_send.at[half, stage],
            recv_sem=ag_recv.at[half, stage, piece % 2],
            device_id={"dp": me + bit * (1 - 2 * bit_of(me, bit))},
            device_id_type=MESH,
        )

    def own_copy(half, piece):
        return pltpu.make_async_copy(wn.at[half], w_outs[half].at[piece, mine[half]], own_sem.at[half])

    def ag_start(stage, piece):
        for half in range(2):
            ag_copy(half, stage, piece).start()
            if stage == 0:
                own_copy(half, piece).start()

    def ag_finish(stage, piece):
        for half in range(2):
            copy = ag_copy(half, stage, piece)
            copy.wait_send()
            copy.wait_recv()
            if stage == 0:
                own_copy(half, piece).wait()

    def is_wide(piece):
        return jnp.logical_or(piece < CHUNKS, piece >= CHUNKS + 2 * PARTS)

    def layer_of(piece):
        return jnp.where(piece < CHUNKS + PARTS, 1, 0)

    def chunk_of(piece):
        return jnp.where(piece < CHUNKS, piece, piece - CHUNKS - 2 * PARTS)

    def part_of(piece):
        return jnp.where(piece < CHUNKS + PARTS, piece - CHUNKS, piece - CHUNKS - PARTS)

    def opt_copies(piece, out):
        layer = layer_of(piece)
        cols = pl.ds(pl.multiple_of(chunk_of(piece) * c, c), c)
        part = pl.ds(pl.multiple_of(part_of(piece) * e, e), e)
        copies_wide, copies_part = [], []
        for half in range(2):
            here = pl.ds(half * 4 * r, 4 * r)
            for k, (hbm, hbm_out, vmem) in enumerate((((mg_hbm, mu_hbm)[half], (mg_out, mu_out)[half], mo), ((vg_hbm, vu_hbm)[half], (vg_out, vu_out)[half], vo))):
                if out:
                    copies_wide.append((vmem.at[half], hbm_out.at[layer, :, cols], opt_sem.at[half, k]))
                else:
                    copies_wide.append((hbm.at[layer, :, cols], vmem.at[half], opt_sem.at[half, k]))
            for k, (hbm, hbm_out, vmem) in enumerate(((md_hbm, md_out, mo_d), (vd_hbm, vd_out, vo_d))):
                if out:
                    copies_part.append((vmem.at[half], hbm_out.at[layer, here, part], opt_sem.at[half, k]))
                else:
                    copies_part.append((hbm.at[layer, here, part], vmem.at[half], opt_sem.at[half, k]))
            if not out:
                row = pl.multiple_of(me * r, 8)
                copies_wide.append(((wg_hbm, wu_hbm)[half].at[layer, pl.ds(row, r), cols], wo.at[half], opt_sem.at[half, 2]))
                row = pl.multiple_of(me * 8 * r + half * 4 * r, 8)
                copies_part.append((wd_hbm.at[layer, pl.ds(row, 4 * r), part], wo_d.at[half], opt_sem.at[half, 2]))
        return ((is_wide(piece), copies_wide), (jnp.logical_not(is_wide(piece)), copies_part))

    def opt_do(piece, out, start):
        for condition, copies in opt_copies(piece, out):

            @pl.when(condition)
            def _(copies=copies):
                for source, to, sem in copies:
                    copy = pltpu.make_async_copy(source, to, sem)
                    copy.start() if start else copy.wait()

    def opt_step(piece):
        @pl.when(is_wide(piece))
        def _():
            for half in range(2):
                w, m, v = adamw(wo[half].astype(F32), mo[half], vo[half], rs_sum(half, piece))
                wn[half], mo[half], vo[half] = w, m, v

        @pl.when(jnp.logical_not(is_wide(piece)))
        def _():
            for half in range(2):
                g = rs_sum(half, piece)
                for j in range(4):
                    at_rows, at_cols = pl.ds(j * r, r), pl.ds(j * e, e)
                    w, m, v = adamw(
                        wo_d[half, at_rows, :].astype(F32), mo_d[half, at_rows, :], vo_d[half, at_rows, :], g[:, j * e : (j + 1) * e]
                    )
                    wn[half, :, at_cols], mo_d[half, at_rows, :], vo_d[half, at_rows, :] = w, m, v

    def active(piece):
        return jnp.logical_and(piece >= 0, piece < PIECES)

    def service(k, point):
        one, two, three, four = k - 1, k - 2, k - 3, k - 4
        if point == 0:

            @pl.when(active(one))
            def _():
                rs_start(0, one)

            @pl.when(active(three))
            def _():
                ag_finish(0, three)
                ag_start(1, three)
                opt_do(three, True, False)

            @pl.when(active(two))
            def _():
                opt_do(two, False, True)

        if point == 1:

            @pl.when(active(one))
            def _():
                rs_finish(0, one)
                rs_start(1, one)

            @pl.when(active(two))
            def _():
                rs_finish(2, two)
                rs_start(3, two)

            @pl.when(active(three))
            def _():
                ag_finish(1, three)
                ag_start(2, three)

            @pl.when(active(four))
            def _():
                ag_finish(3, four)
                ag_start(4, four)

        if point == 2:

            @pl.when(active(two))
            def _():
                rs_finish(3, two)
                rs_start(4, two)

            @pl.when(active(four))
            def _():
                ag_finish(4, four)

        if point == 3:

            @pl.when(active(one))
            def _():
                rs_finish(1, one)
                rs_start(2, one)

            @pl.when(active(two))
            def _():
                for half in range(2):
                    copy = rs_copy(half, STAGES - 1, two % 2)
                    copy.wait_send()
                    copy.wait_recv()
                opt_do(two, False, False)
                opt_step(two)
                opt_do(two, True, True)
                ag_start(0, two)

            @pl.when(active(three))
            def _():
                ag_finish(2, three)
                ag_start(3, three)

    def w_copy(which, piece):
        layer, at_cols = layer_of(piece), pl.ds(pl.multiple_of(chunk_of(piece) * c, c), c)
        if which == 2:
            return pltpu.make_async_copy(wd_hbm.at[layer, at_cols, :], wd, w_sem.at[2])
        return pltpu.make_async_copy((wg_hbm, wu_hbm)[which].at[layer, :, at_cols], (wg, wu)[which], w_sem.at[which])

    def p_copy(piece, tile):
        slot = tile % 2
        at_cols = pl.ds(pl.multiple_of(chunk_of(piece) * c, c), c)
        return pltpu.make_async_copy(ps.at[slot], p1_hbm.at[pl.ds(pl.multiple_of(tile * rows, rows), rows), at_cols], p_sem.at[slot])

    def front_tile(piece, tile):
        here = pl.ds(pl.multiple_of(tile * rows, rows), rows)
        at_, dh_ = a[here, :], dh[here, :]
        @pl.when(jnp.logical_and(layer_of(piece) == 1, tile >= 2))
        def _():
            p_copy(piece, tile - 2).wait()

        n = c // FRONT
        for j in range(FRONT):
            cols = slice(j * n, (j + 1) * n)
            gate, up = dot(at_, wg[:, cols]), dot(at_, wu[:, cols])
            dp = dot(dh_, wd[cols, :], NT).astype(BF).astype(F32)
            s = sigmoid(gate)
            gs = gate * s
            ps[tile % 2, :, cols] = (gs * up).astype(BF)
            du[here, cols] = (dp * gs).astype(BF)
            dg[here, cols] = (dp * up * (s * (1.0 + gate * (1.0 - s)))).astype(BF)

        @pl.when(layer_of(piece) == 1)
        def _():
            p_copy(piece, tile).start()

    def weight_part(which, piece):
        grads, to = (dg, du)[which], (ga, gb)[which]

        @pl.when(layer_of(piece) == 1)
        def _():
            def back(tile, _):
                here = pl.ds(pl.multiple_of(tile * rows, rows), rows)
                part = dot(grads[here, :], (wg, wu)[which][...], NT)
                if which == 0:
                    old = jnp.where(chunk_of(piece) == 0, jnp.zeros_like(part), da[here, :])
                    da[here, :] = old + part
                else:
                    da[here, :] += part
                return 0

            lax.fori_loop(0, tiles, back, 0)

        following = jnp.where(piece < CHUNKS - 1, piece + 1, jnp.where(piece < CHUNKS, CHUNKS + 2 * PARTS, piece + 1))

        @pl.when(following < PIECES)
        def _():
            w_copy(which, following).start()
            if which == 1:
                w_copy(2, following).start()

        n = c // 2
        for j in range(2):
            term = dot(at[...], grads[:, j * n : (j + 1) * n])
            for i in range(32):
                to[piece % 2, place(i, ORDERS[which]), :, j * n : (j + 1) * n] = term[i * r : (i + 1) * r, :].astype(BF)

    def tile_copy(piece, tile, source):
        return pltpu.make_async_copy(source.at[:, pl.ds(tile * wide, wide)], (dg, du)[tile % 2].at[:, pl.ds(0, wide)], load_sem.at[tile % 2])

    def tile_start(piece, tile):
        @pl.when(layer_of(piece) == 1)
        def _():
            tile_copy(piece, tile, p1_hbm).start()

        @pl.when(layer_of(piece) == 0)
        def _():
            tile_copy(piece, tile, p0_hbm).start()

    def down_tile(piece, tile):
        tile_copy(piece, tile, p0_hbm).wait()
        at_rows = pl.ds(pl.multiple_of(part_of(piece) * e, e), e)
        term = dot(dht[at_rows, :], (dg, du)[tile % 2][:, :wide]).T
        for i in range(4):
            for j in range(8):
                half, jj = j // 4, j % 4
                block = term[(8 * i + j) * r : (8 * i + j + 1) * r, :].astype(BF)
                g_bufs[half][piece % 2, place(4 * tile + i, ORDERS[half]), :, jj * e : (jj + 1) * e] = block
        if tile + 2 < 8:
            tile_start(piece, tile + 2)

    def through_norm():
        def back(tile, _):
            here = pl.ds(pl.multiple_of(tile * rows, rows), rows)
            load = pltpu.make_async_copy(h_hbm.at[here, :], ps.at[0, :, pl.ds(0, d)], p_sem.at[0])
            load.start()
            load.wait()

            def some(i, _):
                at_rows = pl.ds(pl.multiple_of(i * 32, 32), 32)
                at_all = pl.ds(pl.multiple_of(tile * rows + i * 32, 32), 32)
                h = ps[0, at_rows, pl.ds(0, d)].astype(F32)
                by_a = da[at_all, :].astype(BF).astype(F32)
                scale = lax.rsqrt(jnp.mean(h * h, -1, keepdims=True) + 1e-6)
                along = jnp.sum(by_a * h, -1, keepdims=True)
                by_h = (by_a * scale - h * (scale * scale * scale * along * (1.0 / d))).astype(BF)
                dh[at_all, :] = (dh[at_all, :].astype(F32) + by_h.astype(F32)).astype(BF)
                return 0

            lax.fori_loop(0, rows // 32, some, 0)
            return 0

        lax.fori_loop(0, tiles, back, 0)

    def turn(source, to):
        def back(tile, _):
            here = pl.ds(pl.multiple_of(tile * rows, rows), rows)
            to[:, here] = source[here, :].astype(F32).T.astype(BF)
            return 0

        lax.fori_loop(0, tiles, back, 0)

    def norm_all():
        def back(i, _):
            here = pl.ds(pl.multiple_of(i * 32, 32), 32)
            a[here, :] = normed(a[here, :])
            return 0

        lax.fori_loop(0, tokens // 32, back, 0)
        turn(a, at)

    first = (
        pltpu.make_async_copy(h_hbm, a, load_sem.at[2]),
        pltpu.make_async_copy(dy_hbm, dh, load_sem.at[3]),
        *(w_copy(which, 0) for which in range(3)),
    )
    for copy in first:
        copy.start()
    first[0].wait()
    norm_all()
    first[1].wait()
    turn(dh, dht)
    x_copy = pltpu.make_async_copy(x_hbm, a, load_sem.at[2])

    def tick(k, _):
        computes = k < PIECES
        gated = jnp.logical_and(computes, is_wide(k))
        downs = jnp.logical_and(computes, jnp.logical_not(is_wide(k)))

        @pl.when(downs)
        def _():
            tile_start(k, 0)
            tile_start(k, 1)

        for point in range(4):
            service(k, point)

            @pl.when(gated)
            def _(point=point):
                if point == 0:
                    for which in range(3):
                        w_copy(which, k).wait()
                if point < 2:

                    def front(i, _):
                        front_tile(k, i + point * (tiles // 2))
                        return 0

                    lax.fori_loop(0, tiles // 2, front, 0)
                else:
                    weight_part(point - 2, k)
                if point == 3:

                    @pl.when(layer_of(k) == 1)
                    def _():
                        p_copy(k, tiles - 2).wait()
                        p_copy(k, tiles - 1).wait()

            @pl.when(downs)
            def _(point=point):
                down_tile(k, 2 * point)
                down_tile(k, 2 * point + 1)

        @pl.when(k == CHUNKS - 1)
        def _():
            x_copy.start()

        @pl.when(k == CHUNKS + PARTS - 1)
        def _():
            through_norm()
            turn(dh, dht)
            x_copy.wait()
            norm_all()

        return 0

    lax.fori_loop(0, PIECES + 4, tick, 0)


def train_step(x, dy, h, p0, weights, ms, vs):
    tokens, d = dy.shape
    ff = p0.shape[1]
    c, r, e = ff // CHUNKS, d // 32, d // PARTS
    rows = min(512, tokens // 4)
    any_ = pl.BlockSpec(memory_space=pl.ANY)
    blocks = lambda *n: pltpu.VMEM((*n, r, c), BF)
    scratch = [
        pltpu.VMEM((tokens, d), BF), pltpu.VMEM((d, tokens), BF), pltpu.VMEM((tokens, d), BF), pltpu.VMEM((d, tokens), BF),
        pltpu.VMEM((d, c), BF), pltpu.VMEM((d, c), BF), pltpu.VMEM((c, d), BF),
        pltpu.VMEM((tokens, c), BF), pltpu.VMEM((tokens, c), BF),
        pltpu.VMEM((2, rows, c), BF),
        pltpu.VMEM((tokens, d), F32),
        blocks(2, 32), blocks(2, 32),
        *[blocks(2, 16 >> s) for s in range(STAGES)] * 2,
        *[blocks(16 >> s) for s in range(STAGES - 1)] * 2,
        blocks(2), pltpu.VMEM((2, r, c), F32), pltpu.VMEM((2, r, c), F32), blocks(2),
        pltpu.VMEM((2, 4 * r, e), F32), pltpu.VMEM((2, 4 * r, e), F32), pltpu.VMEM((2, 4 * r, e), BF),
        pltpu.SemaphoreType.DMA((2, STAGES)), pltpu.SemaphoreType.DMA((2, STAGES, 2)),
        pltpu.SemaphoreType.DMA((2, STAGES)), pltpu.SemaphoreType.DMA((2, STAGES, 2)),
        pltpu.SemaphoreType.DMA((2,)), pltpu.SemaphoreType.DMA((4,)), pltpu.SemaphoreType.DMA((3,)), pltpu.SemaphoreType.DMA((2,)),
        pltpu.SemaphoreType.DMA((2, 3)),
    ]
    packed = jax.ShapeDtypeStruct((PIECES, 32, r, c), BF)
    like = [jax.ShapeDtypeStruct(t.shape, F32) for t in (*ms, *vs)]
    return pl.pallas_call(
        step_kernel,
        name="step",
        in_specs=[any_] * 13,
        out_specs=[any_] * 9,
        out_shape=[packed, packed, *like, jax.ShapeDtypeStruct((tokens, ff), BF)],
        scratch_shapes=scratch,
        compiler_params=pltpu.CompilerParams(collective_id=0, has_side_effects=True, vmem_limit_bytes=67_000_000),
        cost_estimate=pl.CostEstimate(flops=28 * tokens * d * ff, bytes_accessed=400 << 20, transcendentals=0),
    )(x, dy, h, p0, *weights, *ms, *vs)


def unpack_kernel(gate_ref, up_ref, down_a, down_b, wg_ref, wu_ref, wd_ref):
    r, c = gate_ref.shape[-2:]
    e = c // 4
    for core in range(2):
        for z0 in range(2):
            for z1 in range(2):
                owner = z1 * 4 + z0 * 2 + core
                for chunk in range(CHUNKS):
                    at_cols = pl.ds(chunk * c, c)
                    wg_ref[pl.ds(owner * r, r), at_cols] = gate_ref[chunk, core, z0, z1]
                    wu_ref[pl.ds(owner * r, r), at_cols] = up_ref[chunk, core, z0, z1]
                for part in range(PARTS):
                    for half, ref in enumerate((down_a, down_b)):
                        for j in range(4):
                            at_rows = pl.ds(owner * 8 * r + (half * 4 + j) * r, r)
                            wd_ref[at_rows, pl.ds(part * e, e)] = ref[part, core, z0, z1, :, pl.ds(j * e, e)]


def unpack(wa, wb, d, ff):
    r, c = wa.shape[-2:]
    wa, wb = (t.reshape(PIECES, *(2,) * 5, r, c) for t in (wa, wb))
    block = (None, 2, None, 2, r, c)

    def spec(n, first, half):
        def index(layer, x, y):
            outer, inner = (x, y) if half == 0 else (y, x)
            return (first(layer), 0, outer, 0, inner, 0, 0, 0)

        return pl.BlockSpec((n, 2, None, 2, None, 2, r, c), index)

    wide, part = lambda layer: 2 - 2 * layer, lambda layer: 3 - layer
    return pl.pallas_call(
        unpack_kernel,
        name="unpack",
        grid=(2, 2, 2),
        in_specs=[spec(CHUNKS, wide, 0), spec(CHUNKS, wide, 1), spec(PARTS, part, 0), spec(PARTS, part, 1)],
        out_specs=[
            pl.BlockSpec((None, d // 4, ff), lambda layer, x, y: (layer, 2 * x + y, 0)),
            pl.BlockSpec((None, d // 4, ff), lambda layer, x, y: (layer, 2 * x + y, 0)),
            pl.BlockSpec((None, ff // 4, d), lambda layer, x, y: (layer, 2 * x + y, 0)),
        ],
        out_shape=[jax.ShapeDtypeStruct((2, d, ff), BF)] * 2 + [jax.ShapeDtypeStruct((2, ff, d), BF)],
        compiler_params=pltpu.CompilerParams(vmem_limit_bytes=60 << 20),
    )(wa, wb, wa, wb)


def solution(mesh):
    def step(x, dy, *arrays):
        wg, wu, wd = arrays[:3]
        ms, vs = arrays[3:6], arrays[6:9]
        x, dy = x[0], dy[0]
        p0, h = forward(x, wg, wu, wd, 0)
        wa, wb, *moments, _ = train_step(x, dy, h, p0, (wg, wu, wd), ms, vs)
        return (*unpack(wa, wb, x.shape[1], wg.shape[2]), *moments)

    seq, whole, rows = P(("rep", "dp")), P(), P(None, "dp")
    return jax.shard_map(
        step,
        mesh=mesh,
        in_specs=(seq, seq) + (whole,) * 3 + (rows,) * 6,
        out_specs=(P("rep"),) * 3 + (P("rep", "dp"),) * 6,
        check_vma=False,
    )
```

```python
import functools

import jax
import jax.numpy as jnp
from jax import lax
from jax.experimental import pallas as pl
from jax.experimental.pallas import tpu as pltpu
from jax.sharding import PartitionSpec as P

BF = jnp.bfloat16
F32 = jnp.float32
MESH = pl.DeviceIdType.MESH
NN, NT = ((1,), (0,)), ((1,), (1,))

CORE, Z0, Z1, Y, X = 1, 2, 4, 8, 16
ORDERS = ((CORE, X, Z0, Y, Z1), (CORE, Y, Z0, X, Z1))
STAGES = 5
CHUNKS = 6
PARTS = 3
PIECES = 2 * (CHUNKS + PARTS)
FRONT = 4
SUBS = 4
TIMES = (
    (4, 5, 7, 9, 11, 12, 13, 14, 16, 19, 23),
    (5, 6, 8, 10, 11, 12, 13, 17, 20, 23, 27),
    (4, 7, 9, 11, 12, 13, 14, 15, 17, 20, 24),
    (6, 8, 10, 12, 13, 14, 15, 16, 19, 22, 24),
)
TICKS = PIECES + max(t[-1] for t in TIMES) // 4


def dot(a, b, dims=NN):
    return lax.dot_general(a, b, (dims, ((), ())), preferred_element_type=F32)


def bit_of(i, bit):
    return (i // bit) % 2


def place(i, order):
    at = 0
    for bit in order:
        at = at * 2 + bit_of(i, bit)
    return at


def sigmoid(x):
    return 1.0 / (1.0 + jnp.exp(-x))


def normed(h):
    wide = h.astype(F32)
    return (wide * lax.rsqrt(jnp.mean(wide**2, -1, keepdims=True) + 1e-6)).astype(BF)


def adamw(w, m, v, g):
    m = 0.9 * m + 0.1 * g
    v = 0.95 * v + 0.05 * g * g
    step = m * lax.rsqrt(v + 1e-8) + 0.1 * w
    return (w - 0.02 * step).astype(BF), m, v


def forward_kernel(x_ref, wg_ref, wu_ref, wd_ref, p_ref, h_ref, a_all, total):
    chunk, tile = pl.program_id(0), pl.program_id(1)
    rows = p_ref.shape[0]
    here = pl.ds(pl.multiple_of(tile * rows, rows), rows)

    @pl.when(chunk == 0)
    def _():
        a_all[here, :] = normed(x_ref[here, :])

    a = a_all[here, :]
    gate, up = dot(a, wg_ref[...]), dot(a, wu_ref[...])
    p = (gate * sigmoid(gate) * up).astype(BF)
    p_ref[...] = p

    @pl.when(chunk == 0)
    def _():
        total[here, :] = dot(p, wd_ref[...])

    @pl.when(chunk > 0)
    def _():
        total[here, :] += dot(p, wd_ref[...])

    @pl.when(chunk == pl.num_programs(0) - 1)
    def _():
        down = total[here, :].astype(BF).astype(F32)
        h_ref[here, :] = (x_ref[here, :].astype(F32) + down).astype(BF)


def forward(x, wg, wu, wd, layer):
    tokens, d = x.shape
    ff = wg.shape[-1]
    c, rows = ff // CHUNKS, min(512, tokens)
    return pl.pallas_call(
        forward_kernel,
        name="forward",
        grid=(CHUNKS, tokens // rows),
        in_specs=[
            pl.BlockSpec((tokens, d), lambda i, t: (0, 0)),
            pl.BlockSpec((None, d, c), lambda i, t: (layer, 0, i)),
            pl.BlockSpec((None, d, c), lambda i, t: (layer, 0, i)),
            pl.BlockSpec((None, c, d), lambda i, t: (layer, i, 0)),
        ],
        out_specs=[pl.BlockSpec((rows, c), lambda i, t: (t, i)), pl.BlockSpec((tokens, d), lambda i, t: (0, 0))],
        out_shape=[jax.ShapeDtypeStruct((tokens, ff), BF), jax.ShapeDtypeStruct((tokens, d), BF)],
        scratch_shapes=[pltpu.VMEM((tokens, d), BF), pltpu.VMEM((tokens, d), F32)],
        compiler_params=pltpu.CompilerParams(vmem_limit_bytes=60 << 20),
        cost_estimate=pl.CostEstimate(flops=6 * tokens * d * ff, bytes_accessed=60 << 20, transcendentals=0),
    )(x, wg, wu, wd)


def step_kernel(
    x_hbm, dy_hbm, h_hbm, p0_hbm, wg_hbm, wu_hbm, wd_hbm, mg_hbm, mu_hbm, md_hbm, vg_hbm, vu_hbm, vd_hbm,
    wa_out, wb_out, mg_out, mu_out, md_out, vg_out, vu_out, vd_out, p1_hbm,
    a, at, dh, dht, wg, wu, wd, dg, du, ps, da, ga, gb, *rest,
):
    (ra, rb, sa, sb), rest = (rest[0:5], rest[5:10], rest[10:14], rest[14:18]), rest[18:]
    wn, mo, vo, wo, *rest = rest
    rs_send, rs_recv, ag_send, ag_recv, own_sem, load_sem, w_sem, p_sem, opt_sem = rest

    tokens, d = a.shape
    c = wg.shape[1]
    r = d // 32
    e = d // PARTS
    rows = ps.shape[1]
    tiles = tokens // rows
    wide = 4 * 8 * r
    me = lax.axis_index("dp")
    g_bufs, r_bufs, s_bufs, w_outs = (ga, gb), (ra, rb), (sa, sb), (wa_out, wb_out)
    mine = [place(me, order) for order in ORDERS]

    barrier = pltpu.get_barrier_semaphore()
    for bit in (CORE, Z0, Z1, Y, X):
        other = me + bit * (1 - 2 * bit_of(me, bit))
        pl.semaphore_signal(barrier, inc=1, device_id={"dp": other}, device_id_type=MESH)
    pl.semaphore_wait(barrier, 5)

    def rs_copy(half, stage, piece, sub):
        bit = ORDERS[half][stage]
        own, n = bit_of(me, bit), 16 >> stage
        source = g_bufs[half].at[piece % 2, sub] if stage == 0 else s_bufs[half][stage - 1].at[sub]
        return pltpu.make_async_remote_copy(
            src_ref=source.at[pl.ds((1 - own) * n, n)],
            dst_ref=r_bufs[half][stage].at[piece % 2, sub],
            send_sem=rs_send.at[half, stage, sub],
            recv_sem=rs_recv.at[half, stage, sub, piece % 2],
            device_id={"dp": me + bit * (1 - 2 * own)},
            device_id_type=MESH,
        )

    def rs_start(stage, piece, sub):
        for half in range(2):
            rs_copy(half, stage, piece, sub).start()

    def rs_wait(stage, piece, sub):
        for half in range(2):
            copy = rs_copy(half, stage, piece, sub)
            copy.wait_send()
            copy.wait_recv()

    def rs_add(stage, piece, sub):
        n = 16 >> stage
        some = min(n, 4)
        for half in range(2):
            own = bit_of(me, ORDERS[half][stage])
            source = g_bufs[half].at[piece % 2, sub] if stage == 0 else s_bufs[half][stage - 1].at[sub]
            got, to = r_bufs[half][stage].at[piece % 2, sub], s_bufs[half][stage].at[sub]

            def add(i, _, source=source, got=got, to=to, own=own):
                here = pl.ds(i * some, some)
                to[here] = (source[pl.ds(own * n + i * some, some)].astype(F32) + got[here].astype(F32)).astype(BF)
                return 0

            lax.fori_loop(0, n // some, add, 0)

    def rs_sum(half, piece, sub):
        stage = STAGES - 1
        own = bit_of(me, ORDERS[half][stage])
        total = s_bufs[half][stage - 1][sub, own].astype(F32) + r_bufs[half][stage][piece % 2, sub, 0].astype(F32)
        return total.astype(BF).astype(F32)

    def ag_copy(half, stage, piece, sub):
        bit = ORDERS[half][STAGES - 1 - stage]
        n = 1 << stage
        if stage == 0:
            source, to = wn.at[half, sub], w_outs[half].at[piece, sub, mine[half]]
        else:
            source = to = w_outs[half].at[piece, sub, pl.ds((mine[half] // n) * n, n)]
        return pltpu.make_async_remote_copy(
            src_ref=source,
            dst_ref=to,
            send_sem=ag_send.at[half, stage, sub],
            recv_sem=ag_recv.at[half, stage, sub, piece % 2],
            device_id={"dp": me + bit * (1 - 2 * bit_of(me, bit))},
            device_id_type=MESH,
        )

    def own_copy(half, piece, sub):
        return pltpu.make_async_copy(wn.at[half, sub], w_outs[half].at[piece, sub, mine[half]], own_sem.at[half, sub])

    def ag_start(stage, piece, sub):
        for half in range(2):
            ag_copy(half, stage, piece, sub).start()
            if stage == 0:
                own_copy(half, piece, sub).start()

    def ag_finish(stage, piece, sub):
        for half in range(2):
            copy = ag_copy(half, stage, piece, sub)
            copy.wait_send()
            copy.wait_recv()
            if stage == 0:
                own_copy(half, piece, sub).wait()

    def is_wide(piece):
        return jnp.logical_or(piece < CHUNKS, piece >= CHUNKS + 2 * PARTS)

    def layer_of(piece):
        return jnp.where(piece < CHUNKS + PARTS, 1, 0)

    def chunk_of(piece):
        return jnp.where(piece < CHUNKS, piece, piece - CHUNKS - 2 * PARTS)

    def part_of(piece):
        return jnp.where(piece < CHUNKS + PARTS, piece - CHUNKS, piece - CHUNKS - PARTS)

    def opt_do(piece, sub, out, start):
        layer = layer_of(piece)
        wide_cols = pl.ds(pl.multiple_of(chunk_of(piece) * c + sub * e, e), e)
        part_cols = pl.ds(pl.multiple_of(part_of(piece) * e, e), e)

        def copies(wide):
            for half in range(2):
                group = (half * SUBS + sub) * r
                rows_, cols = (slice(None), wide_cols) if wide else (pl.ds(group, r), part_cols)
                kinds = ((mg_hbm, mu_hbm)[half], mg_out if half == 0 else mu_out, mo), ((vg_hbm, vu_hbm)[half], vg_out if half == 0 else vu_out, vo)
                if not wide:
                    kinds = (md_hbm, md_out, mo), (vd_hbm, vd_out, vo)
                for k, (hbm, hbm_out, vmem) in enumerate(kinds):
                    sem = opt_sem.at[half, k, sub]
                    if out:
                        yield pltpu.make_async_copy(vmem.at[half, sub], hbm_out.at[layer, rows_, cols], sem)
                    else:
                        yield pltpu.make_async_copy(hbm.at[layer, rows_, cols], vmem.at[half, sub], sem)
                if not out:
                    own = me * r if wide else me * 8 * r + group
                    source = (wg_hbm, wu_hbm)[half] if wide else wd_hbm
                    own = pl.ds(pl.multiple_of(own, 8), r)
                    yield pltpu.make_async_copy(source.at[layer, own, cols], wo.at[half, sub], opt_sem.at[half, 2, sub])

        if not start:
            for half in range(2):
                for k, vmem in enumerate((mo, vo, wo)[: 2 if out else 3]):
                    block = (mg_hbm, vg_hbm, wg_hbm)[k].at[0, pl.ds(0, r), pl.ds(0, e)]
                    pltpu.make_async_copy(block, vmem.at[half, sub], opt_sem.at[half, k, sub]).wait()
            return
        for wide in (True, False):

            @pl.when(is_wide(piece) == wide)
            def _(wide=wide):
                for copy in copies(wide):
                    copy.start()

    def opt_step(piece, sub):
        for half in range(2):
            w, m, v = adamw(wo[half, sub].astype(F32), mo[half, sub], vo[half, sub], rs_sum(half, piece, sub))
            wn[half, sub], mo[half, sub], vo[half, sub] = w, m, v

    def go_on(event, piece, sub):
        if event < STAGES:
            if event >= 0:
                rs_wait(event, piece, sub)
            if 0 <= event < STAGES - 1:
                rs_add(event, piece, sub)
            if event < STAGES - 1:
                rs_start(event + 1, piece, sub)
            if event == STAGES - 2:
                opt_do(piece, sub, False, True)
            if event == STAGES - 1:
                opt_do(piece, sub, False, False)
                opt_step(piece, sub)
                opt_do(piece, sub, True, True)
                ag_start(0, piece, sub)
        else:
            ag_finish(event - STAGES, piece, sub)
            if event == STAGES:
                opt_do(piece, sub, True, False)
            if event < 2 * STAGES - 1:
                ag_start(event - STAGES + 1, piece, sub)

    def service(k, point):
        due = [(event - 1, sub, at) for sub in range(SUBS) for event, at in enumerate(TIMES[sub]) if at % 4 == point]
        for event, sub, at in sorted(due, key=lambda one: (-one[0], -one[2], one[1])):
            piece = k - at // 4

            @pl.when(jnp.logical_and(piece >= 0, piece < PIECES))
            def _(event=event, piece=piece, sub=sub):
                go_on(event, piece, sub)

    def w_copy(which, piece):
        layer, at_cols = layer_of(piece), pl.ds(pl.multiple_of(chunk_of(piece) * c, c), c)
        if which == 2:
            return pltpu.make_async_copy(wd_hbm.at[layer, at_cols, :], wd, w_sem.at[2])
        return pltpu.make_async_copy((wg_hbm, wu_hbm)[which].at[layer, :, at_cols], (wg, wu)[which], w_sem.at[which])

    def p_copy(piece, tile):
        slot = tile % 2
        at_cols = pl.ds(pl.multiple_of(chunk_of(piece) * c, c), c)
        return pltpu.make_async_copy(ps.at[slot], p1_hbm.at[pl.ds(pl.multiple_of(tile * rows, rows), rows), at_cols], p_sem.at[slot])

    def front_tile(piece, tile):
        here = pl.ds(pl.multiple_of(tile * rows, rows), rows)
        at_, dh_ = a[here, :], dh[here, :]
        @pl.when(jnp.logical_and(layer_of(piece) == 1, tile >= 2))
        def _():
            p_copy(piece, tile - 2).wait()

        n = c // FRONT
        for j in range(FRONT):
            cols = slice(j * n, (j + 1) * n)
            gate, up = dot(at_, wg[:, cols]), dot(at_, wu[:, cols])
            dp = dot(dh_, wd[cols, :], NT).astype(BF).astype(F32)
            s = sigmoid(gate)
            gs = gate * s
            ps[tile % 2, :, cols] = (gs * up).astype(BF)
            du[here, cols] = (dp * gs).astype(BF)
            dg[here, cols] = (dp * up * (s * (1.0 + gate * (1.0 - s)))).astype(BF)

        @pl.when(layer_of(piece) == 1)
        def _():
            p_copy(piece, tile).start()

    def weight_part(which, piece):
        grads = (dg, du)[which]

        @pl.when(layer_of(piece) == 1)
        def _():
            def back(tile, _):
                here = pl.ds(pl.multiple_of(tile * rows, rows), rows)
                part = dot(grads[here, :], (wg, wu)[which][...], NT)
                if which == 0:
                    old = jnp.where(chunk_of(piece) == 0, jnp.zeros_like(part), da[here, :])
                    da[here, :] = old + part
                else:
                    da[here, :] += part
                return 0

            lax.fori_loop(0, tiles, back, 0)

        following = jnp.where(piece < CHUNKS - 1, piece + 1, jnp.where(piece < CHUNKS, CHUNKS + 2 * PARTS, piece + 1))

        @pl.when(following < PIECES)
        def _():
            w_copy(which, following).start()
            if which == 1:
                w_copy(2, following).start()

        for which_, (grads_, to) in enumerate(((dg, ga), (du, gb))):
            n = c // 2
            term = dot(at[...], grads_[:, which * n : (which + 1) * n])
            for i in range(32):
                for sub in range(SUBS // 2):
                    block = term[i * r : (i + 1) * r, sub * e : (sub + 1) * e].astype(BF)
                    to[piece % 2, which * (SUBS // 2) + sub, place(i, ORDERS[which_])] = block

    def tile_copy(piece, tile, source):
        return pltpu.make_async_copy(source.at[:, pl.ds(tile * wide, wide)], (dg, du)[tile % 2].at[:, pl.ds(0, wide)], load_sem.at[tile % 2])

    def tile_start(piece, tile):
        @pl.when(layer_of(piece) == 1)
        def _():
            tile_copy(piece, tile, p1_hbm).start()

        @pl.when(layer_of(piece) == 0)
        def _():
            tile_copy(piece, tile, p0_hbm).start()

    def down_tile(piece, tile):
        tile_copy(piece, tile, p0_hbm).wait()
        at_rows = pl.ds(pl.multiple_of(part_of(piece) * e, e), e)
        term = dot(dht[at_rows, :], (dg, du)[tile % 2][:, :wide]).T
        for i in range(4):
            for j in range(8):
                half, sub = j // SUBS, j % SUBS
                block = term[(8 * i + j) * r : (8 * i + j + 1) * r, :].astype(BF)
                g_bufs[half][piece % 2, sub, place(4 * tile + i, ORDERS[half])] = block
        if tile + 2 < 8:
            tile_start(piece, tile + 2)

    def through_norm():
        def back(tile, _):
            here = pl.ds(pl.multiple_of(tile * rows, rows), rows)
            load = pltpu.make_async_copy(h_hbm.at[here, :], ps.at[0, :, pl.ds(0, d)], p_sem.at[0])
            load.start()
            load.wait()

            def some(i, _):
                at_rows = pl.ds(pl.multiple_of(i * 32, 32), 32)
                at_all = pl.ds(pl.multiple_of(tile * rows + i * 32, 32), 32)
                h = ps[0, at_rows, pl.ds(0, d)].astype(F32)
                by_a = da[at_all, :].astype(BF).astype(F32)
                scale = lax.rsqrt(jnp.mean(h * h, -1, keepdims=True) + 1e-6)
                along = jnp.sum(by_a * h, -1, keepdims=True)
                by_h = (by_a * scale - h * (scale * scale * scale * along * (1.0 / d))).astype(BF)
                dh[at_all, :] = (dh[at_all, :].astype(F32) + by_h.astype(F32)).astype(BF)
                return 0

            lax.fori_loop(0, rows // 32, some, 0)
            return 0

        lax.fori_loop(0, tiles, back, 0)

    def turn(source, to):
        def back(tile, _):
            here = pl.ds(pl.multiple_of(tile * rows, rows), rows)
            to[:, here] = source[here, :].astype(F32).T.astype(BF)
            return 0

        lax.fori_loop(0, tiles, back, 0)

    def norm_all():
        def back(i, _):
            here = pl.ds(pl.multiple_of(i * 32, 32), 32)
            a[here, :] = normed(a[here, :])
            return 0

        lax.fori_loop(0, tokens // 32, back, 0)
        turn(a, at)

    first = (
        pltpu.make_async_copy(h_hbm, a, load_sem.at[2]),
        pltpu.make_async_copy(dy_hbm, dh, load_sem.at[3]),
        *(w_copy(which, 0) for which in range(3)),
    )
    for copy in first:
        copy.start()
    first[0].wait()
    norm_all()
    first[1].wait()
    turn(dh, dht)
    x_copy = pltpu.make_async_copy(x_hbm, a, load_sem.at[2])

    def tick(k, _):
        computes = k < PIECES
        gated = jnp.logical_and(computes, is_wide(k))
        downs = jnp.logical_and(computes, jnp.logical_not(is_wide(k)))

        @pl.when(downs)
        def _():
            tile_start(k, 0)
            tile_start(k, 1)

        for point in range(4):
            service(k, point)

            @pl.when(gated)
            def _(point=point):
                if point == 0:
                    for which in range(3):
                        w_copy(which, k).wait()
                if point < 2:

                    def front(i, _):
                        front_tile(k, i + point * (tiles // 2))
                        return 0

                    lax.fori_loop(0, tiles // 2, front, 0)
                else:
                    weight_part(point - 2, k)
                if point == 3:

                    @pl.when(layer_of(k) == 1)
                    def _():
                        p_copy(k, tiles - 2).wait()
                        p_copy(k, tiles - 1).wait()

            @pl.when(downs)
            def _(point=point):
                down_tile(k, 2 * point)
                down_tile(k, 2 * point + 1)

        @pl.when(k == CHUNKS - 1)
        def _():
            x_copy.start()

        @pl.when(k == CHUNKS + PARTS - 1)
        def _():
            through_norm()
            turn(dh, dht)
            x_copy.wait()
            norm_all()

        return 0

    lax.fori_loop(0, TICKS, tick, 0)


def train_step(x, dy, h, p0, weights, ms, vs):
    tokens, d = dy.shape
    ff = p0.shape[1]
    c, r, e = ff // CHUNKS, d // 32, d // PARTS
    rows = min(512, tokens // 4)
    any_ = pl.BlockSpec(memory_space=pl.ANY)
    blocks = lambda *n: pltpu.VMEM((*n, r, e), BF)
    scratch = [
        pltpu.VMEM((tokens, d), BF), pltpu.VMEM((d, tokens), BF), pltpu.VMEM((tokens, d), BF), pltpu.VMEM((d, tokens), BF),
        pltpu.VMEM((d, c), BF), pltpu.VMEM((d, c), BF), pltpu.VMEM((c, d), BF),
        pltpu.VMEM((tokens, c), BF), pltpu.VMEM((tokens, c), BF),
        pltpu.VMEM((2, rows, c), BF),
        pltpu.VMEM((tokens, d), F32),
        blocks(2, SUBS, 32), blocks(2, SUBS, 32),
        *[blocks(2, SUBS, 16 >> s) for s in range(STAGES)] * 2,
        *[blocks(SUBS, 16 >> s) for s in range(STAGES - 1)] * 2,
        blocks(2, SUBS), pltpu.VMEM((2, SUBS, r, e), F32), pltpu.VMEM((2, SUBS, r, e), F32), blocks(2, SUBS),
        pltpu.SemaphoreType.DMA((2, STAGES, SUBS)), pltpu.SemaphoreType.DMA((2, STAGES, SUBS, 2)),
        pltpu.SemaphoreType.DMA((2, STAGES, SUBS)), pltpu.SemaphoreType.DMA((2, STAGES, SUBS, 2)),
        pltpu.SemaphoreType.DMA((2, SUBS)), pltpu.SemaphoreType.DMA((4,)), pltpu.SemaphoreType.DMA((3,)), pltpu.SemaphoreType.DMA((2,)),
        pltpu.SemaphoreType.DMA((2, 3, SUBS)),
    ]
    packed = jax.ShapeDtypeStruct((PIECES, SUBS, 32, r, e), BF)
    like = [jax.ShapeDtypeStruct(t.shape, F32) for t in (*ms, *vs)]
    return pl.pallas_call(
        step_kernel,
        name="step",
        in_specs=[any_] * 13,
        out_specs=[any_] * 9,
        out_shape=[packed, packed, *like, jax.ShapeDtypeStruct((tokens, ff), BF)],
        scratch_shapes=scratch,
        compiler_params=pltpu.CompilerParams(collective_id=0, has_side_effects=True, vmem_limit_bytes=67_000_000),
        cost_estimate=pl.CostEstimate(flops=28 * tokens * d * ff, bytes_accessed=400 << 20, transcendentals=0),
    )(x, dy, h, p0, *weights, *ms, *vs)


def unpack_kernel(gate_ref, up_ref, down_a, down_b, *refs):
    r, e = gate_ref.shape[-2:]
    moments, (wg_ref, wu_ref, wd_ref), moments_out = refs[:6], refs[6:9], refs[9:]
    for source, to in zip(moments, moments_out, strict=True):
        to[...] = source[...]
    for core in range(2):
        for z0 in range(2):
            for z1 in range(2):
                owner = z1 * 4 + z0 * 2 + core
                for sub in range(SUBS):
                    for chunk in range(CHUNKS):
                        at_rows, at_cols = pl.ds(owner * r, r), pl.ds((chunk * SUBS + sub) * e, e)
                        wg_ref[at_rows, at_cols] = gate_ref[chunk, sub, core, z0, z1]
                        wu_ref[at_rows, at_cols] = up_ref[chunk, sub, core, z0, z1]
                    for part in range(PARTS):
                        for half, ref in enumerate((down_a, down_b)):
                            at_rows = pl.ds((owner * 8 + half * SUBS + sub) * r, r)
                            wd_ref[at_rows, pl.ds(part * e, e)] = ref[part, sub, core, z0, z1]


def unpack(wa, wb, moments, d, ff):
    r, e = wa.shape[-2:]
    wa, wb = (t.reshape(PIECES, SUBS, *(2,) * 5, r, e) for t in (wa, wb))

    def spec(n, first, half):
        def index(layer, x, y):
            outer, inner = (x, y) if half == 0 else (y, x)
            return (first(layer), 0, 0, outer, 0, inner, 0, 0, 0)

        return pl.BlockSpec((n, SUBS, 2, None, 2, None, 2, r, e), index)

    wide, part = lambda layer: 2 - 2 * layer, lambda layer: 3 - layer
    slab = lambda rows, cols: pl.BlockSpec((None, rows, cols), lambda layer, x, y: (layer, 2 * x + y, 0))
    moment = [
        pl.BlockSpec((None, r, ff // 4), lambda layer, x, y: (layer, 0, 2 * x + y)) if t.shape[2] == ff else slab(2 * r, d) for t in moments
    ]
    return pl.pallas_call(
        unpack_kernel,
        name="unpack",
        grid=(2, 2, 2),
        in_specs=[spec(CHUNKS, wide, 0), spec(CHUNKS, wide, 1), spec(PARTS, part, 0), spec(PARTS, part, 1), *moment],
        out_specs=[slab(d // 4, ff), slab(d // 4, ff), slab(ff // 4, d), *moment],
        out_shape=[jax.ShapeDtypeStruct((2, d, ff), BF)] * 2
        + [jax.ShapeDtypeStruct((2, ff, d), BF)]
        + [jax.ShapeDtypeStruct(t.shape, F32) for t in moments],
        compiler_params=pltpu.CompilerParams(vmem_limit_bytes=60 << 20),
    )(wa, wb, wa, wb, *moments)


def solution(mesh):
    def step(x, dy, *arrays):
        wg, wu, wd = arrays[:3]
        ms, vs = arrays[3:6], arrays[6:9]
        x, dy = x[0], dy[0]
        p0, h = forward(x, wg, wu, wd, 0)
        wa, wb, *moments, _ = train_step(x, dy, h, p0, (wg, wu, wd), ms, vs)
        return tuple(unpack(wa, wb, moments, x.shape[1], wg.shape[2]))

    seq, whole, rows = P(("rep", "dp")), P(), P(None, "dp")
    return jax.shard_map(
        step,
        mesh=mesh,
        in_specs=(seq, seq) + (whole,) * 3 + (rows,) * 6,
        out_specs=(P("rep"),) * 3 + (P("rep", "dp"),) * 6,
        check_vma=False,
    )
```

```python
import functools

import jax
import jax.numpy as jnp
from jax import lax
from jax.experimental import pallas as pl
from jax.experimental.pallas import tpu as pltpu
from jax.sharding import PartitionSpec as P

BF = jnp.bfloat16
F32 = jnp.float32
MESH = pl.DeviceIdType.MESH
NN, NT = ((1,), (0,)), ((1,), (1,))

CORE, Z0, Z1, Y, X = 1, 2, 4, 8, 16
ORDERS = ((CORE, X, Z0, Y, Z1), (CORE, Y, Z0, X, Z1))
STAGES = 5
CHUNKS = 6
PARTS = 3
PIECES = 2 * (CHUNKS + PARTS)
FRONT = 4
STRIP = 32
SUBS = 4
POINTS = 8
TIMES = (
    (8, 10, 15, 19, 21, 24, 26, 30, 35, 42, 49),
    (10, 14, 18, 22, 24, 26, 29, 33, 39, 46, 49),
    (11, 16, 22, 26, 29, 31, 33, 40, 45, 52, 58),
    (9, 11, 19, 23, 25, 27, 31, 36, 41, 48, 56),
)
TICKS = PIECES + max(t[-1] for t in TIMES) // POINTS


def dot(a, b, dims=NN):
    return lax.dot_general(a, b, (dims, ((), ())), preferred_element_type=F32)


def bit_of(i, bit):
    return (i // bit) % 2


def place(i, order):
    at = 0
    for bit in order:
        at = at * 2 + bit_of(i, bit)
    return at


def sigmoid(x):
    return 1.0 / (1.0 + jnp.exp(-x))


def normed(h):
    wide = h.astype(F32)
    return (wide * lax.rsqrt(jnp.mean(wide**2, -1, keepdims=True) + 1e-6)).astype(BF)


def adamw(w, m, v, g):
    m = 0.9 * m + 0.1 * g
    v = 0.95 * v + 0.05 * g * g
    step = m * lax.rsqrt(v + 1e-8) + 0.1 * w
    return (w - 0.02 * step).astype(BF), m, v


def forward_kernel(x_ref, wg_ref, wu_ref, wd_ref, p_ref, h_ref, a_all, total):
    chunk, tile = pl.program_id(0), pl.program_id(1)
    rows = p_ref.shape[0]
    here = pl.ds(pl.multiple_of(tile * rows, rows), rows)

    @pl.when(chunk == 0)
    def _():
        a_all[here, :] = normed(x_ref[here, :])

    a = a_all[here, :]
    gate, up = dot(a, wg_ref[...]), dot(a, wu_ref[...])
    p = (gate * sigmoid(gate) * up).astype(BF)
    p_ref[...] = p

    @pl.when(chunk == 0)
    def _():
        total[here, :] = dot(p, wd_ref[...])

    @pl.when(chunk > 0)
    def _():
        total[here, :] += dot(p, wd_ref[...])

    @pl.when(chunk == pl.num_programs(0) - 1)
    def _():
        down = total[here, :].astype(BF).astype(F32)
        h_ref[here, :] = (x_ref[here, :].astype(F32) + down).astype(BF)


def forward(x, wg, wu, wd, layer):
    tokens, d = x.shape
    ff = wg.shape[-1]
    c, rows = ff // CHUNKS, min(512, tokens)
    return pl.pallas_call(
        forward_kernel,
        name="forward",
        grid=(CHUNKS, tokens // rows),
        in_specs=[
            pl.BlockSpec((tokens, d), lambda i, t: (0, 0)),
            pl.BlockSpec((None, d, c), lambda i, t: (layer, 0, i)),
            pl.BlockSpec((None, d, c), lambda i, t: (layer, 0, i)),
            pl.BlockSpec((None, c, d), lambda i, t: (layer, i, 0)),
        ],
        out_specs=[pl.BlockSpec((rows, c), lambda i, t: (t, i)), pl.BlockSpec((tokens, d), lambda i, t: (0, 0))],
        out_shape=[jax.ShapeDtypeStruct((tokens, ff), BF), jax.ShapeDtypeStruct((tokens, d), BF)],
        scratch_shapes=[pltpu.VMEM((tokens, d), BF), pltpu.VMEM((tokens, d), F32)],
        compiler_params=pltpu.CompilerParams(vmem_limit_bytes=60 << 20),
        cost_estimate=pl.CostEstimate(flops=6 * tokens * d * ff, bytes_accessed=60 << 20, transcendentals=0),
    )(x, wg, wu, wd)


def step_kernel(
    x_hbm, dy_hbm, h_hbm, p0_hbm, wg_hbm, wu_hbm, wd_hbm, mg_hbm, mu_hbm, md_hbm, vg_hbm, vu_hbm, vd_hbm,
    wa_out, wb_out, mg_out, mu_out, md_out, vg_out, vu_out, vd_out, p1_hbm, dg_hbm, du_hbm,
    a, at, dh, dht, wg, wu, wd, dg, du, ps, da, ga, gb, *rest,
):
    (ra, rb, sa, sb), rest = (rest[0:5], rest[5:10], rest[10:14], rest[14:18]), rest[18:]
    wn, mo, vo, wo, *rest = rest
    rs_send, rs_recv, ag_send, ag_recv, own_sem, load_sem, w_sem, p_sem, opt_sem, d_sem = rest

    tokens, d = a.shape
    c = wg.shape[1]
    r = d // 32
    e = d // PARTS
    rows = ps.shape[1]
    tiles = tokens // rows
    wide = 4 * 8 * r
    me = lax.axis_index("dp")
    g_bufs, r_bufs, s_bufs, w_outs = (ga, gb), (ra, rb), (sa, sb), (wa_out, wb_out)
    mine = [place(me, order) for order in ORDERS]

    barrier = pltpu.get_barrier_semaphore()
    for bit in (CORE, Z0, Z1, Y, X):
        other = me + bit * (1 - 2 * bit_of(me, bit))
        pl.semaphore_signal(barrier, inc=1, device_id={"dp": other}, device_id_type=MESH)
    pl.semaphore_wait(barrier, 5)

    def rs_copy(half, stage, piece, sub):
        bit = ORDERS[half][stage]
        own, n = bit_of(me, bit), 16 >> stage
        source = g_bufs[half].at[piece % 2, sub] if stage == 0 else s_bufs[half][stage - 1].at[sub]
        return pltpu.make_async_remote_copy(
            src_ref=source.at[pl.ds((1 - own) * n, n)],
            dst_ref=r_bufs[half][stage].at[piece % 2, sub],
            send_sem=rs_send.at[half, stage, sub],
            recv_sem=rs_recv.at[half, stage, sub, piece % 2],
            device_id={"dp": me + bit * (1 - 2 * own)},
            device_id_type=MESH,
        )

    def rs_start(stage, piece, sub):
        for half in range(2):
            rs_copy(half, stage, piece, sub).start()

    def rs_wait(stage, piece, sub):
        for half in range(2):
            copy = rs_copy(half, stage, piece, sub)
            copy.wait_send()
            copy.wait_recv()

    def rs_add(stage, piece, sub):
        n = 16 >> stage
        some = min(n, 4)
        for half in range(2):
            own = bit_of(me, ORDERS[half][stage])
            source = g_bufs[half].at[piece % 2, sub] if stage == 0 else s_bufs[half][stage - 1].at[sub]
            got, to = r_bufs[half][stage].at[piece % 2, sub], s_bufs[half][stage].at[sub]

            def add(i, _, source=source, got=got, to=to, own=own):
                here = pl.ds(i * some, some)
                to[here] = (source[pl.ds(own * n + i * some, some)].astype(F32) + got[here].astype(F32)).astype(BF)
                return 0

            lax.fori_loop(0, n // some, add, 0)

    def rs_sum(half, piece, sub):
        stage = STAGES - 1
        own = bit_of(me, ORDERS[half][stage])
        total = s_bufs[half][stage - 1][sub, own].astype(F32) + r_bufs[half][stage][piece % 2, sub, 0].astype(F32)
        return total.astype(BF).astype(F32)

    def ag_copy(half, stage, piece, sub):
        bit = ORDERS[half][STAGES - 1 - stage]
        n = 1 << stage
        if stage == 0:
            source, to = wn.at[half, sub], w_outs[half].at[piece, sub, mine[half]]
        else:
            source = to = w_outs[half].at[piece, sub, pl.ds((mine[half] // n) * n, n)]
        return pltpu.make_async_remote_copy(
            src_ref=source,
            dst_ref=to,
            send_sem=ag_send.at[half, stage, sub],
            recv_sem=ag_recv.at[half, stage, sub, piece % 2],
            device_id={"dp": me + bit * (1 - 2 * bit_of(me, bit))},
            device_id_type=MESH,
        )

    def own_copy(half, piece, sub):
        return pltpu.make_async_copy(wn.at[half, sub], w_outs[half].at[piece, sub, mine[half]], own_sem.at[half, sub])

    def ag_start(stage, piece, sub):
        for half in range(2):
            ag_copy(half, stage, piece, sub).start()
            if stage == 0:
                own_copy(half, piece, sub).start()

    def ag_finish(stage, piece, sub):
        for half in range(2):
            copy = ag_copy(half, stage, piece, sub)
            copy.wait_send()
            copy.wait_recv()
            if stage == 0:
                own_copy(half, piece, sub).wait()

    def is_wide(piece):
        return jnp.logical_or(piece < CHUNKS, piece >= CHUNKS + 2 * PARTS)

    def layer_of(piece):
        return jnp.where(piece < CHUNKS + PARTS, 1, 0)

    def chunk_of(piece):
        return jnp.where(piece < CHUNKS, piece, piece - CHUNKS - 2 * PARTS)

    def part_of(piece):
        return jnp.where(piece < CHUNKS + PARTS, piece - CHUNKS, piece - CHUNKS - PARTS)

    def opt_do(piece, sub, out, start):
        layer = layer_of(piece)
        wide_cols = pl.ds(pl.multiple_of(chunk_of(piece) * c + sub * e, e), e)
        part_cols = pl.ds(pl.multiple_of(part_of(piece) * e, e), e)

        def copies(wide):
            for half in range(2):
                group = (half * SUBS + sub) * r
                rows_, cols = (slice(None), wide_cols) if wide else (pl.ds(group, r), part_cols)
                kinds = ((mg_hbm, mu_hbm)[half], mg_out if half == 0 else mu_out, mo), ((vg_hbm, vu_hbm)[half], vg_out if half == 0 else vu_out, vo)
                if not wide:
                    kinds = (md_hbm, md_out, mo), (vd_hbm, vd_out, vo)
                for k, (hbm, hbm_out, vmem) in enumerate(kinds):
                    sem = opt_sem.at[half, k, sub]
                    if out:
                        yield pltpu.make_async_copy(vmem.at[half, sub], hbm_out.at[layer, rows_, cols], sem)
                    else:
                        yield pltpu.make_async_copy(hbm.at[layer, rows_, cols], vmem.at[half, sub], sem)
                if not out:
                    own = me * r if wide else me * 8 * r + group
                    source = (wg_hbm, wu_hbm)[half] if wide else wd_hbm
                    own = pl.ds(pl.multiple_of(own, 8), r)
                    yield pltpu.make_async_copy(source.at[layer, own, cols], wo.at[half, sub], opt_sem.at[half, 2, sub])

        if not start:
            for half in range(2):
                for k, vmem in enumerate((mo, vo, wo)[: 2 if out else 3]):
                    block = (mg_hbm, vg_hbm, wg_hbm)[k].at[0, pl.ds(0, r), pl.ds(0, e)]
                    pltpu.make_async_copy(block, vmem.at[half, sub], opt_sem.at[half, k, sub]).wait()
            return
        for wide in (True, False):

            @pl.when(is_wide(piece) == wide)
            def _(wide=wide):
                for copy in copies(wide):
                    copy.start()

    def opt_step(piece, sub):
        for half in range(2):
            w, m, v = adamw(wo[half, sub].astype(F32), mo[half, sub], vo[half, sub], rs_sum(half, piece, sub))
            wn[half, sub], mo[half, sub], vo[half, sub] = w, m, v

    def go_on(event, piece, sub):
        if event < STAGES:
            if event >= 0:
                rs_wait(event, piece, sub)
            if 0 <= event < STAGES - 1:
                rs_add(event, piece, sub)
            if event < STAGES - 1:
                rs_start(event + 1, piece, sub)
            if event == STAGES - 2:
                opt_do(piece, sub, False, True)
            if event == STAGES - 1:
                opt_do(piece, sub, False, False)
                opt_step(piece, sub)
                opt_do(piece, sub, True, True)
                ag_start(0, piece, sub)
        else:
            ag_finish(event - STAGES, piece, sub)
            if event == STAGES:
                opt_do(piece, sub, True, False)
            if event < 2 * STAGES - 1:
                ag_start(event - STAGES + 1, piece, sub)

    def service(k, point):
        due = [(event - 1, sub, at) for sub in range(SUBS) for event, at in enumerate(TIMES[sub]) if at % POINTS == point]
        for event, sub, at in sorted(due, key=lambda one: (-one[0], -one[2], one[1])):
            piece = k - at // POINTS

            @pl.when(jnp.logical_and(piece >= 0, piece < PIECES))
            def _(event=event, piece=piece, sub=sub):
                go_on(event, piece, sub)

    def w_copy(which, layer, chunk):
        at_cols = pl.ds(pl.multiple_of(chunk * c, c), c)
        if which == 2:
            return pltpu.make_async_copy(wd_hbm.at[layer, at_cols, :], wd, w_sem.at[2])
        return pltpu.make_async_copy((wg_hbm, wu_hbm)[which].at[layer, :, at_cols], (wg, wu)[which], w_sem.at[which])

    def p_copy(piece, tile):
        slot = tile % 2
        at_cols = pl.ds(pl.multiple_of(chunk_of(piece) * c, c), c)
        return pltpu.make_async_copy(ps.at[slot], p1_hbm.at[pl.ds(pl.multiple_of(tile * rows, rows), rows), at_cols], p_sem.at[slot])

    def d_copy(which, chunk, tile, load):
        here = pl.ds(pl.multiple_of(tile * rows, rows), rows)
        vmem, hbm = (dg, du)[which].at[here, :], (dg_hbm, du_hbm)[which].at[here, pl.ds(pl.multiple_of(chunk * c, c), c)]
        return pltpu.make_async_copy(*((hbm, vmem) if load else (vmem, hbm)), d_sem.at[which, tile])

    def front_tile(piece, tile):
        here = pl.ds(pl.multiple_of(tile * rows, rows), rows)
        at_, dh_ = a[here, :], dh[here, :]
        @pl.when(jnp.logical_and(layer_of(piece) == 1, tile >= 2))
        def _():
            p_copy(piece, tile - 2).wait()

        n = c // FRONT
        for j in range(FRONT):
            cols = slice(j * n, (j + 1) * n)
            gates, ups = dot(at_, wg[:, cols]), dot(at_, wu[:, cols])
            dps = dot(dh_, wd[cols, :], NT)
            for i in range(0, rows, STRIP):
                gate, up = gates[i : i + STRIP], ups[i : i + STRIP]
                dp = dps[i : i + STRIP].astype(BF).astype(F32)
                s = sigmoid(gate)
                gs = gate * s
                out = pl.ds(pl.multiple_of(tile * rows + i, STRIP), STRIP)
                ps[tile % 2, i : i + STRIP, cols] = (gs * up).astype(BF)
                du[out, cols] = (dp * gs).astype(BF)
                dg[out, cols] = (dp * up * (s + gs * (1.0 - s))).astype(BF)

        @pl.when(layer_of(piece) == 1)
        def _():
            p_copy(piece, tile).start()
            for which in range(2):
                d_copy(which, chunk_of(piece), tile, False).start()

    def weight_part(side, which, piece):
        n = c // 2
        term = dot(at[...], (dg, du)[which][:, side * n : (side + 1) * n])
        for i in range(32):
            for sub in range(SUBS // 2):
                block = term[i * r : (i + 1) * r, sub * e : (sub + 1) * e].astype(BF)
                (ga, gb)[which][piece % 2, side * (SUBS // 2) + sub, place(i, ORDERS[which])] = block

    def through_layer(which, chunk, more):
        w_copy(which, 1, chunk).wait()

        def back(tile, _):
            here = pl.ds(pl.multiple_of(tile * rows, rows), rows)
            d_copy(which, chunk, tile, True).wait()
            part = dot((dg, du)[which][here, :], (wg, wu)[which][...], NT)
            if which == 0:
                da[here, :] = jnp.where(chunk == 0, jnp.zeros_like(part), da[here, :]) + part
            else:
                da[here, :] += part
            if more:
                d_copy(which, chunk + 1, tile, True).start()
            return 0

        lax.fori_loop(0, tiles, back, 0)
        if more:
            w_copy(which, 1, chunk + 1).start()

    def tile_copy(piece, tile, source):
        return pltpu.make_async_copy(source.at[:, pl.ds(tile * wide, wide)], (dg, du)[tile % 2].at[:, pl.ds(0, wide)], load_sem.at[tile % 2])

    def tile_start(piece, tile):
        @pl.when(layer_of(piece) == 1)
        def _():
            tile_copy(piece, tile, p1_hbm).start()

        @pl.when(layer_of(piece) == 0)
        def _():
            tile_copy(piece, tile, p0_hbm).start()

    def down_tile(piece, tile):
        tile_copy(piece, tile, p0_hbm).wait()
        at_rows = pl.ds(pl.multiple_of(part_of(piece) * e, e), e)
        term = dot(dht[at_rows, :], (dg, du)[tile % 2][:, :wide]).T
        for i in range(4):
            for j in range(8):
                half, sub = j // SUBS, j % SUBS
                block = term[(8 * i + j) * r : (8 * i + j + 1) * r, :].astype(BF)
                g_bufs[half][piece % 2, sub, place(4 * tile + i, ORDERS[half])] = block
        if tile + 2 < 8:
            tile_start(piece, tile + 2)

    def through_norm():
        def back(tile, _):
            here = pl.ds(pl.multiple_of(tile * rows, rows), rows)
            load = pltpu.make_async_copy(h_hbm.at[here, :], ps.at[0, :, pl.ds(0, d)], p_sem.at[0])
            load.start()
            load.wait()

            def some(i, _):
                at_rows = pl.ds(pl.multiple_of(i * 32, 32), 32)
                at_all = pl.ds(pl.multiple_of(tile * rows + i * 32, 32), 32)
                h = ps[0, at_rows, pl.ds(0, d)].astype(F32)
                by_a = da[at_all, :].astype(BF).astype(F32)
                scale = lax.rsqrt(jnp.mean(h * h, -1, keepdims=True) + 1e-6)
                along = jnp.sum(by_a * h, -1, keepdims=True)
                by_h = (by_a * scale - h * (scale * scale * scale * along * (1.0 / d))).astype(BF)
                dh[at_all, :] = (dh[at_all, :].astype(F32) + by_h.astype(F32)).astype(BF)
                return 0

            lax.fori_loop(0, rows // 32, some, 0)
            return 0

        lax.fori_loop(0, tiles, back, 0)

    def turn(source, to):
        def back(tile, _):
            here = pl.ds(pl.multiple_of(tile * rows, rows), rows)
            to[:, here] = source[here, :].astype(F32).T.astype(BF)
            return 0

        lax.fori_loop(0, tiles, back, 0)

    def norm_all():
        def back(i, _):
            here = pl.ds(pl.multiple_of(i * 32, 32), 32)
            a[here, :] = normed(a[here, :])
            return 0

        lax.fori_loop(0, tokens // 32, back, 0)
        turn(a, at)

    first = (
        pltpu.make_async_copy(h_hbm, a, load_sem.at[2]),
        pltpu.make_async_copy(dy_hbm, dh, load_sem.at[3]),
        *(w_copy(which, 1, 0) for which in range(3)),
    )
    for copy in first:
        copy.start()
    first[0].wait()
    norm_all()
    first[1].wait()
    turn(dh, dht)
    x_copy = pltpu.make_async_copy(x_hbm, a, load_sem.at[2])

    def tick(k, _):
        computes = k < PIECES
        gated = jnp.logical_and(computes, is_wide(k))
        downs = jnp.logical_and(computes, jnp.logical_not(is_wide(k)))
        downs_1 = jnp.logical_and(downs, layer_of(k) == 1)

        @pl.when(downs)
        def _():
            tile_start(k, 0)
            tile_start(k, 1)

        @pl.when(downs_1)
        def _():
            for which in range(2):
                w_copy(which, 1, 2 * part_of(k)).start()

        for point in range(POINTS):
            service(k, point)

            @pl.when(gated)
            def _(point=point):
                if point == 0:
                    for which in range(3):
                        w_copy(which, layer_of(k), chunk_of(k)).wait()
                if point < 4:
                    front_tile(k, point)
                else:
                    weight_part(point // 2 - 2, point % 2, k)
                if point == 3:
                    @pl.when(jnp.logical_and(k != CHUNKS - 1, k < PIECES - 1))
                    def _():
                        for which in range(3):
                            w_copy(which, layer_of(k), chunk_of(k) + 1).start()

                if point == POINTS - 1:

                    @pl.when(layer_of(k) == 1)
                    def _():
                        p_copy(k, tiles - 2).wait()
                        p_copy(k, tiles - 1).wait()
                        for which in range(2):
                            for tile in range(tiles):
                                d_copy(which, chunk_of(k), tile, False).wait()

            if point < 4:

                @pl.when(downs)
                def _(point=point):
                    down_tile(k, 2 * point)
                    down_tile(k, 2 * point + 1)

            else:

                @pl.when(downs_1)
                def _(point=point):
                    if point == 4:
                        for tile in range(tiles):
                            for which in range(2):
                                d_copy(which, 2 * part_of(k), tile, True).start()
                    through_layer(point % 2, 2 * part_of(k) + point // 2 - 2, point < 6)

        @pl.when(k == CHUNKS - 1)
        def _():
            x_copy.start()

        @pl.when(k == CHUNKS + PARTS - 1)
        def _():
            for which in range(3):
                w_copy(which, 0, 0).start()
            through_norm()
            turn(dh, dht)
            x_copy.wait()
            norm_all()

        return 0

    lax.fori_loop(0, TICKS, tick, 0)


def train_step(x, dy, h, p0, weights, ms, vs):
    tokens, d = dy.shape
    ff = p0.shape[1]
    c, r, e = ff // CHUNKS, d // 32, d // PARTS
    rows = min(512, tokens // 4)
    any_ = pl.BlockSpec(memory_space=pl.ANY)
    blocks = lambda *n: pltpu.VMEM((*n, r, e), BF)
    scratch = [
        pltpu.VMEM((tokens, d), BF), pltpu.VMEM((d, tokens), BF), pltpu.VMEM((tokens, d), BF), pltpu.VMEM((d, tokens), BF),
        pltpu.VMEM((d, c), BF), pltpu.VMEM((d, c), BF), pltpu.VMEM((c, d), BF),
        pltpu.VMEM((tokens, c), BF), pltpu.VMEM((tokens, c), BF),
        pltpu.VMEM((2, rows, c), BF),
        pltpu.VMEM((tokens, d), F32),
        blocks(2, SUBS, 32), blocks(2, SUBS, 32),
        *[blocks(2, SUBS, 16 >> s) for s in range(STAGES)] * 2,
        *[blocks(SUBS, 16 >> s) for s in range(STAGES - 1)] * 2,
        blocks(2, SUBS), pltpu.VMEM((2, SUBS, r, e), F32), pltpu.VMEM((2, SUBS, r, e), F32), blocks(2, SUBS),
        pltpu.SemaphoreType.DMA((2, STAGES, SUBS)), pltpu.SemaphoreType.DMA((2, STAGES, SUBS, 2)),
        pltpu.SemaphoreType.DMA((2, STAGES, SUBS)), pltpu.SemaphoreType.DMA((2, STAGES, SUBS, 2)),
        pltpu.SemaphoreType.DMA((2, SUBS)), pltpu.SemaphoreType.DMA((4,)), pltpu.SemaphoreType.DMA((3,)), pltpu.SemaphoreType.DMA((2,)),
        pltpu.SemaphoreType.DMA((2, 3, SUBS)), pltpu.SemaphoreType.DMA((2, 4)),
    ]
    packed = jax.ShapeDtypeStruct((PIECES, SUBS, 32, r, e), BF)
    like = [jax.ShapeDtypeStruct(t.shape, F32) for t in (*ms, *vs)]
    return pl.pallas_call(
        step_kernel,
        name="step",
        in_specs=[any_] * 13,
        out_specs=[any_] * 11,
        out_shape=[packed, packed, *like, *[jax.ShapeDtypeStruct((tokens, ff), BF)] * 3],
        scratch_shapes=scratch,
        compiler_params=pltpu.CompilerParams(collective_id=0, has_side_effects=True, vmem_limit_bytes=67_000_000),
        cost_estimate=pl.CostEstimate(flops=28 * tokens * d * ff, bytes_accessed=400 << 20, transcendentals=0),
    )(x, dy, h, p0, *weights, *ms, *vs)


def unpack_kernel(gate_ref, up_ref, down_a, down_b, *refs):
    r, e = gate_ref.shape[-2:]
    moments, (wg_ref, wu_ref, wd_ref), moments_out = refs[:6], refs[6:9], refs[9:]
    for source, to in zip(moments, moments_out, strict=True):
        to[...] = source[...]
    for core in range(2):
        for z0 in range(2):
            for z1 in range(2):
                owner = z1 * 4 + z0 * 2 + core
                for sub in range(SUBS):
                    for chunk in range(CHUNKS):
                        at_rows, at_cols = pl.ds(owner * r, r), pl.ds((chunk * SUBS + sub) * e, e)
                        wg_ref[at_rows, at_cols] = gate_ref[chunk, sub, core, z0, z1]
                        wu_ref[at_rows, at_cols] = up_ref[chunk, sub, core, z0, z1]
                    for part in range(PARTS):
                        for half, ref in enumerate((down_a, down_b)):
                            at_rows = pl.ds((owner * 8 + half * SUBS + sub) * r, r)
                            wd_ref[at_rows, pl.ds(part * e, e)] = ref[part, sub, core, z0, z1]


def unpack(wa, wb, moments, d, ff):
    r, e = wa.shape[-2:]
    wa, wb = (t.reshape(PIECES, SUBS, *(2,) * 5, r, e) for t in (wa, wb))

    def spec(n, first, half):
        def index(layer, x, y):
            outer, inner = (x, y) if half == 0 else (y, x)
            return (first(layer), 0, 0, outer, 0, inner, 0, 0, 0)

        return pl.BlockSpec((n, SUBS, 2, None, 2, None, 2, r, e), index)

    wide, part = lambda layer: 2 - 2 * layer, lambda layer: 3 - layer
    slab = lambda rows, cols: pl.BlockSpec((None, rows, cols), lambda layer, x, y: (layer, 2 * x + y, 0))
    moment = [
        pl.BlockSpec((None, r, ff // 4), lambda layer, x, y: (layer, 0, 2 * x + y)) if t.shape[2] == ff else slab(2 * r, d) for t in moments
    ]
    return pl.pallas_call(
        unpack_kernel,
        name="unpack",
        grid=(2, 2, 2),
        in_specs=[spec(CHUNKS, wide, 0), spec(CHUNKS, wide, 1), spec(PARTS, part, 0), spec(PARTS, part, 1), *moment],
        out_specs=[slab(d // 4, ff), slab(d // 4, ff), slab(ff // 4, d), *moment],
        out_shape=[jax.ShapeDtypeStruct((2, d, ff), BF)] * 2
        + [jax.ShapeDtypeStruct((2, ff, d), BF)]
        + [jax.ShapeDtypeStruct(t.shape, F32) for t in moments],
        compiler_params=pltpu.CompilerParams(vmem_limit_bytes=60 << 20),
    )(wa, wb, wa, wb, *moments)


def solution(mesh):
    def step(x, dy, *arrays):
        wg, wu, wd = arrays[:3]
        ms, vs = arrays[3:6], arrays[6:9]
        x, dy = x[0], dy[0]
        p0, h = forward(x, wg, wu, wd, 0)
        wa, wb, *moments, _, _, _ = train_step(x, dy, h, p0, (wg, wu, wd), ms, vs)
        return tuple(unpack(wa, wb, moments, x.shape[1], wg.shape[2]))

    seq, whole, rows = P(("rep", "dp")), P(), P(None, "dp")
    return jax.shard_map(
        step,
        mesh=mesh,
        in_specs=(seq, seq) + (whole,) * 3 + (rows,) * 6,
        out_specs=(P("rep"),) * 3 + (P("rep", "dp"),) * 6,
        check_vma=False,
    )
```

```python
import functools

import jax
import jax.numpy as jnp
from jax import lax
from jax.experimental import pallas as pl
from jax.experimental.pallas import tpu as pltpu
from jax.sharding import PartitionSpec as P

BF = jnp.bfloat16
F32 = jnp.float32
MESH = pl.DeviceIdType.MESH
NN, NT = ((1,), (0,)), ((1,), (1,))

CORE, Z0, Z1, Y, X = 1, 2, 4, 8, 16
ORDERS = ((CORE, X, Z0, Y, Z1), (CORE, Y, Z0, X, Z1))
STAGES = 5
CHUNKS = 6
PARTS = 3
PIECES = 2 * (CHUNKS + PARTS)
FRONT = 4
STRIP = 32
SUBS = 2
GROUPS = 4 // SUBS
POINTS = 8
TIMES = (
    (8, 9, 13, 17, 20, 24, 28, 31, 38, 44, 48),
    (10, 11, 15, 21, 23, 26, 31, 35, 40, 47, 55),
)
TICKS = PIECES + max(t[-1] for t in TIMES) // POINTS


def dot(a, b, dims=NN):
    return lax.dot_general(a, b, (dims, ((), ())), preferred_element_type=F32)


def bit_of(i, bit):
    return (i // bit) % 2


def place(i, order):
    at = 0
    for bit in order:
        at = at * 2 + bit_of(i, bit)
    return at


def sigmoid(x):
    return 1.0 / (1.0 + jnp.exp(-x))


def normed(h):
    wide = h.astype(F32)
    return (wide * lax.rsqrt(jnp.mean(wide**2, -1, keepdims=True) + 1e-6)).astype(BF)


def adamw(w, m, v, g):
    m = 0.9 * m + 0.1 * g
    v = 0.95 * v + 0.05 * g * g
    step = m * lax.rsqrt(v + 1e-8) + 0.1 * w
    return (w - 0.02 * step).astype(BF), m, v


def forward_kernel(x_ref, wg_ref, wu_ref, wd_ref, p_ref, h_ref, gate_ref, up_ref, a_all, total):
    chunk, tile = pl.program_id(0), pl.program_id(1)
    rows = p_ref.shape[0]
    here = pl.ds(pl.multiple_of(tile * rows, rows), rows)

    @pl.when(chunk == 0)
    def _():
        a_all[here, :] = normed(x_ref[here, :])

    a = a_all[here, :]
    gate, up = dot(a, wg_ref[...]), dot(a, wu_ref[...])
    gate_ref[...], up_ref[...] = gate, up
    p = (gate * sigmoid(gate) * up).astype(BF)
    p_ref[...] = p

    @pl.when(chunk == 0)
    def _():
        total[here, :] = dot(p, wd_ref[...])

    @pl.when(chunk > 0)
    def _():
        total[here, :] += dot(p, wd_ref[...])

    @pl.when(chunk == pl.num_programs(0) - 1)
    def _():
        down = total[here, :].astype(BF).astype(F32)
        h_ref[here, :] = (x_ref[here, :].astype(F32) + down).astype(BF)


def forward(x, wg, wu, wd, layer):
    tokens, d = x.shape
    ff = wg.shape[-1]
    c, rows = ff // CHUNKS, min(512, tokens)
    return pl.pallas_call(
        forward_kernel,
        name="forward",
        grid=(CHUNKS, tokens // rows),
        in_specs=[
            pl.BlockSpec((tokens, d), lambda i, t: (0, 0)),
            pl.BlockSpec((None, d, c), lambda i, t: (layer, 0, i)),
            pl.BlockSpec((None, d, c), lambda i, t: (layer, 0, i)),
            pl.BlockSpec((None, c, d), lambda i, t: (layer, i, 0)),
        ],
        out_specs=[
            pl.BlockSpec((rows, c), lambda i, t: (t, i)),
            pl.BlockSpec((tokens, d), lambda i, t: (0, 0)),
            *[pl.BlockSpec((rows, c), lambda i, t: (t, i))] * 2,
        ],
        out_shape=[
            jax.ShapeDtypeStruct((tokens, ff), BF),
            jax.ShapeDtypeStruct((tokens, d), BF),
            *[jax.ShapeDtypeStruct((tokens, ff), F32)] * 2,
        ],
        scratch_shapes=[pltpu.VMEM((tokens, d), BF), pltpu.VMEM((tokens, d), F32)],
        compiler_params=pltpu.CompilerParams(vmem_limit_bytes=60 << 20),
        cost_estimate=pl.CostEstimate(flops=6 * tokens * d * ff, bytes_accessed=60 << 20, transcendentals=0),
    )(x, wg, wu, wd)


def step_kernel(
    x_hbm, dy_hbm, h_hbm, p0_hbm, gate_hbm, up_hbm, wg_hbm, wu_hbm, wd_hbm, mg_hbm, mu_hbm, md_hbm, vg_hbm, vu_hbm, vd_hbm,
    wa_out, wb_out, mg_out, mu_out, md_out, vg_out, vu_out, vd_out, p1_hbm, dg_hbm, du_hbm,
    a, at, dh, dht, wg, wu, wd, dg, du, ps, big, ga, gb, *rest,
):
    (ra, rb, sa, sb), rest = (rest[0:5], rest[5:10], rest[10:14], rest[14:18]), rest[18:]
    wn, mo, vo, wo, *rest = rest
    rs_send, rs_recv, ag_send, ag_recv, own_sem, load_sem, w_sem, p_sem, opt_sem, d_sem, gu_sem = rest

    tokens, d = a.shape
    c = wg.shape[1]
    r = d // 32
    e = d // PARTS
    rows = ps.shape[1]
    tiles = tokens // rows
    wide = 4 * 8 * r
    me = lax.axis_index("dp")
    g_bufs, r_bufs, s_bufs, w_outs = (ga, gb), (ra, rb), (sa, sb), (wa_out, wb_out)
    mine = [place(me, order) for order in ORDERS]

    barrier = pltpu.get_barrier_semaphore()
    for bit in (CORE, Z0, Z1, Y, X):
        other = me + bit * (1 - 2 * bit_of(me, bit))
        pl.semaphore_signal(barrier, inc=1, device_id={"dp": other}, device_id_type=MESH)
    pl.semaphore_wait(barrier, 5)

    def rs_copy(half, stage, piece, sub):
        bit = ORDERS[half][stage]
        own, n = bit_of(me, bit), 16 >> stage
        source = g_bufs[half].at[piece % 2, sub] if stage == 0 else s_bufs[half][stage - 1].at[sub]
        return pltpu.make_async_remote_copy(
            src_ref=source.at[pl.ds((1 - own) * n, n)],
            dst_ref=r_bufs[half][stage].at[piece % 2, sub],
            send_sem=rs_send.at[half, stage, sub],
            recv_sem=rs_recv.at[half, stage, sub, piece % 2],
            device_id={"dp": me + bit * (1 - 2 * own)},
            device_id_type=MESH,
        )

    def rs_start(stage, piece, sub):
        for half in range(2):
            rs_copy(half, stage, piece, sub).start()

    def rs_wait(stage, piece, sub):
        for half in range(2):
            copy = rs_copy(half, stage, piece, sub)
            copy.wait_send()
            copy.wait_recv()

    def rs_add(stage, piece, sub):
        n = 16 >> stage
        some = min(n, SUBS)
        for half in range(2):
            own = bit_of(me, ORDERS[half][stage])
            source = g_bufs[half].at[piece % 2, sub] if stage == 0 else s_bufs[half][stage - 1].at[sub]
            got, to = r_bufs[half][stage].at[piece % 2, sub], s_bufs[half][stage].at[sub]

            def add(i, _, source=source, got=got, to=to, own=own):
                here = pl.ds(i * some, some)
                to[here] = (source[pl.ds(own * n + i * some, some)].astype(F32) + got[here].astype(F32)).astype(BF)
                return 0

            lax.fori_loop(0, n // some, add, 0)

    def rs_sum(half, piece, sub):
        stage = STAGES - 1
        own = bit_of(me, ORDERS[half][stage])
        total = s_bufs[half][stage - 1][sub, own].astype(F32) + r_bufs[half][stage][piece % 2, sub, 0].astype(F32)
        return total.astype(BF).astype(F32)

    def ag_copy(half, stage, piece, sub):
        bit = ORDERS[half][STAGES - 1 - stage]
        n = 1 << stage
        if stage == 0:
            source, to = wn.at[half, sub], w_outs[half].at[piece, sub, mine[half]]
        else:
            source = to = w_outs[half].at[piece, sub, pl.ds((mine[half] // n) * n, n)]
        return pltpu.make_async_remote_copy(
            src_ref=source,
            dst_ref=to,
            send_sem=ag_send.at[half, stage, sub],
            recv_sem=ag_recv.at[half, stage, sub, piece % 2],
            device_id={"dp": me + bit * (1 - 2 * bit_of(me, bit))},
            device_id_type=MESH,
        )

    def own_copy(half, piece, sub):
        return pltpu.make_async_copy(wn.at[half, sub], w_outs[half].at[piece, sub, mine[half]], own_sem.at[half, sub])

    def ag_start(stage, piece, sub):
        for half in range(2):
            ag_copy(half, stage, piece, sub).start()
            if stage == 0:
                own_copy(half, piece, sub).start()

    def ag_finish(stage, piece, sub):
        for half in range(2):
            copy = ag_copy(half, stage, piece, sub)
            copy.wait_send()
            copy.wait_recv()
            if stage == 0:
                own_copy(half, piece, sub).wait()

    def is_wide(piece):
        return jnp.logical_or(piece < CHUNKS, piece >= CHUNKS + 2 * PARTS)

    def layer_of(piece):
        return jnp.where(piece < CHUNKS + PARTS, 1, 0)

    def chunk_of(piece):
        return jnp.where(piece < CHUNKS, piece, piece - CHUNKS - 2 * PARTS)

    def part_of(piece):
        return jnp.where(piece < CHUNKS + PARTS, piece - CHUNKS, piece - CHUNKS - PARTS)

    def opt_do(piece, sub, out, start):
        layer = layer_of(piece)
        part_cols = pl.ds(pl.multiple_of(part_of(piece) * e, e), e)

        def copies(wide):
            for half in range(2):
                for q in range(GROUPS):
                    group = sub * GROUPS + q
                    wide_cols = pl.ds(pl.multiple_of(chunk_of(piece) * c + group * e, e), e)
                    row = (half * 4 + group) * r
                    rows_, cols = (slice(None), wide_cols) if wide else (pl.ds(row, r), part_cols)
                    if wide:
                        kinds = ((mg_hbm, mu_hbm)[half], (mg_out, mu_out)[half], mo), ((vg_hbm, vu_hbm)[half], (vg_out, vu_out)[half], vo)
                    else:
                        kinds = (md_hbm, md_out, mo), (vd_hbm, vd_out, vo)
                    for k, (hbm, hbm_out, vmem) in enumerate(kinds):
                        sem = opt_sem.at[half, k, group]
                        if out:
                            yield pltpu.make_async_copy(vmem.at[half, sub, q], hbm_out.at[layer, rows_, cols], sem)
                        else:
                            yield pltpu.make_async_copy(hbm.at[layer, rows_, cols], vmem.at[half, sub, q], sem)
                    if not out:
                        own = pl.ds(pl.multiple_of(me * r if wide else me * 8 * r + row, 8), r)
                        source = (wg_hbm, wu_hbm)[half] if wide else wd_hbm
                        yield pltpu.make_async_copy(source.at[layer, own, cols], wo.at[half, sub, q], opt_sem.at[half, 2, group])

        if not start:
            for half in range(2):
                for q in range(GROUPS):
                    for k, vmem in enumerate((mo, vo, wo)[: 2 if out else 3]):
                        block = (mg_hbm, vg_hbm, wg_hbm)[k].at[0, pl.ds(0, r), pl.ds(0, e)]
                        pltpu.make_async_copy(block, vmem.at[half, sub, q], opt_sem.at[half, k, sub * GROUPS + q]).wait()
            return
        for wide in (True, False):

            @pl.when(is_wide(piece) == wide)
            def _(wide=wide):
                for copy in copies(wide):
                    copy.start()

    def opt_step(piece, sub):
        for half in range(2):
            w, m, v = adamw(wo[half, sub].astype(F32), mo[half, sub], vo[half, sub], rs_sum(half, piece, sub))
            wn[half, sub], mo[half, sub], vo[half, sub] = w, m, v

    def go_on(event, piece, sub):
        if event < STAGES:
            if event >= 0:
                rs_wait(event, piece, sub)
            if 0 <= event < STAGES - 1:
                rs_add(event, piece, sub)
            if event < STAGES - 1:
                rs_start(event + 1, piece, sub)
            if event == STAGES - 2:
                opt_do(piece, sub, False, True)
            if event == STAGES - 1:
                opt_do(piece, sub, False, False)
                opt_step(piece, sub)
                opt_do(piece, sub, True, True)
                ag_start(0, piece, sub)
        else:
            ag_finish(event - STAGES, piece, sub)
            if event == STAGES:
                opt_do(piece, sub, True, False)
            if event < 2 * STAGES - 1:
                ag_start(event - STAGES + 1, piece, sub)

    def service(k, point):
        due = [(event - 1, sub, at) for sub in range(SUBS) for event, at in enumerate(TIMES[sub]) if at % POINTS == point]
        for event, sub, at in sorted(due, key=lambda one: (-one[0], -one[2], one[1])):
            piece = k - at // POINTS

            @pl.when(jnp.logical_and(piece >= 0, piece < PIECES))
            def _(event=event, piece=piece, sub=sub):
                go_on(event, piece, sub)

    def w_copy(which, layer, chunk):
        at_cols = pl.ds(pl.multiple_of(chunk * c, c), c)
        if which == 2:
            return pltpu.make_async_copy(wd_hbm.at[layer, at_cols, :], wd, w_sem.at[2])
        return pltpu.make_async_copy((wg_hbm, wu_hbm)[which].at[layer, :, at_cols], (wg, wu)[which], w_sem.at[which])

    def p_copy(piece, tile):
        slot = tile % 2
        at_cols = pl.ds(pl.multiple_of(chunk_of(piece) * c, c), c)
        return pltpu.make_async_copy(ps.at[slot], p1_hbm.at[pl.ds(pl.multiple_of(tile * rows, rows), rows), at_cols], p_sem.at[slot])

    def d_copy(which, chunk, tile, load):
        here = pl.ds(pl.multiple_of(tile * rows, rows), rows)
        vmem, hbm = (dg, du)[which].at[here, :], (dg_hbm, du_hbm)[which].at[here, pl.ds(pl.multiple_of(chunk * c, c), c)]
        return pltpu.make_async_copy(*((hbm, vmem) if load else (vmem, hbm)), d_sem.at[which, tile])

    def front_tile(piece, tile):
        here = pl.ds(pl.multiple_of(tile * rows, rows), rows)
        at_, dh_ = a[here, :], dh[here, :]

        @pl.when(tile >= 2)
        def _():
            p_copy(piece, tile - 2).wait()

        n = c // FRONT
        for j in range(FRONT):
            cols = slice(j * n, (j + 1) * n)
            gates, ups = dot(at_, wg[:, cols]), dot(at_, wu[:, cols])
            dps = dot(dh_, wd[cols, :], NT)
            for i in range(0, rows, STRIP):
                gate, up = gates[i : i + STRIP], ups[i : i + STRIP]
                dp = dps[i : i + STRIP].astype(BF).astype(F32)
                s = sigmoid(gate)
                gs = gate * s
                out = pl.ds(pl.multiple_of(tile * rows + i, STRIP), STRIP)
                ps[tile % 2, i : i + STRIP, cols] = (gs * up).astype(BF)
                du[out, cols] = (dp * gs).astype(BF)
                dg[out, cols] = (dp * up * (s + gs * (1.0 - s))).astype(BF)

        p_copy(piece, tile).start()
        for which in range(2):
            d_copy(which, chunk_of(piece), tile, False).start()

    def gu_copy(which, chunk, tile):
        slot = 2 * (tile % 2) + which
        source = (gate_hbm, up_hbm)[which].at[pl.ds(pl.multiple_of(tile * rows, rows), rows), pl.ds(pl.multiple_of(chunk * c, c), c)]
        return pltpu.make_async_copy(source, big.at[:, pl.ds(pl.multiple_of(slot * c, c), c)], gu_sem.at[slot])

    def kept_tile(piece, tile):
        here = pl.ds(pl.multiple_of(tile * rows, rows), rows)
        dh_ = dh[here, :]
        for which in range(2):
            gu_copy(which, chunk_of(piece), tile).wait()
        n = c // FRONT
        for j in range(FRONT):
            cols = slice(j * n, (j + 1) * n)
            dps = dot(dh_, wd[cols, :], NT)
            at_gate, at_up = (pl.ds(pl.multiple_of((2 * (tile % 2) + which) * c + j * n, n), n) for which in range(2))
            for i in range(0, rows, STRIP):
                gate, up = big[i : i + STRIP, at_gate], big[i : i + STRIP, at_up]
                dp = dps[i : i + STRIP].astype(BF).astype(F32)
                s = sigmoid(gate)
                gs = gate * s
                out = pl.ds(pl.multiple_of(tile * rows + i, STRIP), STRIP)
                du[out, cols] = (dp * gs).astype(BF)
                dg[out, cols] = (dp * up * (s + gs * (1.0 - s))).astype(BF)

        following = piece * tiles + tile + 2

        @pl.when(following < PIECES * tiles)
        def _():
            for which in range(2):
                gu_copy(which, following // tiles - CHUNKS - 2 * PARTS, following % tiles).start()

    def weight_part(side, which, piece):
        n = c // 2
        term = dot(at[...], (dg, du)[which][:, pl.ds(pl.multiple_of(side * n, n), n)])
        for i in range(32):
            for q in range(2):
                group = side * 2 + q
                block = term[i * r : (i + 1) * r, q * e : (q + 1) * e].astype(BF)
                (ga, gb)[which][piece % 2, group // GROUPS, place(i, ORDERS[which]), group % GROUPS] = block

    def through_layer(which, piece, side):
        chunk = 2 * part_of(piece) + side
        w_copy(which, 1, chunk).wait()

        def back(tile, _):
            here = pl.ds(pl.multiple_of(tile * rows, rows), rows)
            total = pl.ds(pl.multiple_of(tile * d, 128), d)
            d_copy(which, chunk, tile, True).wait()
            part = dot((dg, du)[which][here, :], (wg, wu)[which][...], NT)
            if which == 0:
                big[:, total] = jnp.where(chunk == 0, jnp.zeros_like(part), big[:, total]) + part
            else:
                big[:, total] += part

            @pl.when(side == 0)
            def _():
                d_copy(which, chunk + 1, tile, True).start()

            return 0

        lax.fori_loop(0, tiles, back, 0)

        @pl.when(side == 0)
        def _():
            w_copy(which, 1, chunk + 1).start()

    def tile_copy(which, tile, source):
        from_cols = pl.ds(pl.multiple_of(tile * wide, 128), wide)
        return pltpu.make_async_copy(source.at[:, from_cols], (dg, du)[which].at[:, pl.ds(0, wide)], load_sem.at[which])

    def tile_start(piece, which, tile):
        for layer, source in enumerate((p0_hbm, p1_hbm)):

            @pl.when(layer_of(piece) == layer)
            def _(source=source):
                tile_copy(which, tile, source).start()

    def down_tile(piece, which, tile):
        tile_copy(which, tile, p0_hbm).wait()
        at_rows = pl.ds(pl.multiple_of(part_of(piece) * e, e), e)
        term = dot(dht[at_rows, :], (dg, du)[which][:, :wide]).T
        for i in range(4):
            for j in range(8):
                half, group = j // 4, j % 4
                block = term[(8 * i + j) * r : (8 * i + j + 1) * r, :].astype(BF)
                g_bufs[half][piece % 2, group // GROUPS, place(4 * tile + i, ORDERS[half]), group % GROUPS] = block

        @pl.when(tile + 2 < 8)
        def _():
            tile_start(piece, which, tile + 2)

    def through_norm():
        def back(tile, _):
            here = pl.ds(pl.multiple_of(tile * rows, rows), rows)
            load = pltpu.make_async_copy(h_hbm.at[here, :], ps.at[0, :, pl.ds(0, d)], p_sem.at[0])
            load.start()
            load.wait()

            def some(i, _):
                at_rows = pl.ds(pl.multiple_of(i * 32, 32), 32)
                at_all = pl.ds(pl.multiple_of(tile * rows + i * 32, 32), 32)
                total = pl.ds(pl.multiple_of(tile * d, 128), d)
                h = ps[0, at_rows, pl.ds(0, d)].astype(F32)
                by_a = big[at_rows, total].astype(BF).astype(F32)
                scale = lax.rsqrt(jnp.mean(h * h, -1, keepdims=True) + 1e-6)
                along = jnp.sum(by_a * h, -1, keepdims=True)
                by_h = (by_a * scale - h * (scale * scale * scale * along * (1.0 / d))).astype(BF)
                dh[at_all, :] = (dh[at_all, :].astype(F32) + by_h.astype(F32)).astype(BF)
                return 0

            lax.fori_loop(0, rows // 32, some, 0)
            return 0

        lax.fori_loop(0, tiles, back, 0)

    def turn(source, to):
        def back(tile, _):
            here = pl.ds(pl.multiple_of(tile * rows, rows), rows)
            to[:, here] = source[here, :].astype(F32).T.astype(BF)
            return 0

        lax.fori_loop(0, tiles, back, 0)

    def norm_all():
        def back(i, _):
            here = pl.ds(pl.multiple_of(i * 32, 32), 32)
            a[here, :] = normed(a[here, :])
            return 0

        lax.fori_loop(0, tokens // 32, back, 0)
        turn(a, at)

    first = (
        pltpu.make_async_copy(h_hbm, a, load_sem.at[2]),
        pltpu.make_async_copy(dy_hbm, dh, load_sem.at[3]),
        *(w_copy(which, 1, 0) for which in range(3)),
    )
    for copy in first:
        copy.start()
    first[0].wait()
    norm_all()
    first[1].wait()
    turn(dh, dht)
    x_copy = pltpu.make_async_copy(x_hbm, a, load_sem.at[2])

    def tick(k, _):
        computes = k < PIECES
        layer = layer_of(k)
        gated = jnp.logical_and(computes, is_wide(k))
        downs = jnp.logical_and(computes, jnp.logical_not(is_wide(k)))
        downs_1 = jnp.logical_and(downs, layer == 1)

        @pl.when(downs)
        def _():
            tile_start(k, 0, 0)
            tile_start(k, 1, 1)

        @pl.when(downs_1)
        def _():
            for which in range(2):
                w_copy(which, 1, 2 * part_of(k)).start()

        def serve(point, points):
            for one in points:

                @pl.when(point == one)
                def _(one=one):
                    service(k, one)

        def fronts(point, _):
            serve(point, range(4))

            @pl.when(jnp.logical_and(gated, layer == 1))
            def _():
                @pl.when(point == 0)
                def _():
                    for which in range(3):
                        w_copy(which, 1, chunk_of(k)).wait()

                front_tile(k, point)

            @pl.when(jnp.logical_and(gated, layer == 0))
            def _():
                @pl.when(point == 0)
                def _():
                    w_copy(2, 0, chunk_of(k)).wait()

                kept_tile(k, point)

            @pl.when(downs)
            def _():
                for which in range(2):
                    down_tile(k, which, 2 * point + which)

            return 0

        lax.fori_loop(0, 4, fronts, 0)

        @pl.when(k < CHUNKS - 1)
        def _():
            for which in range(3):
                w_copy(which, 1, chunk_of(k) + 1).start()

        @pl.when(jnp.logical_and(k >= CHUNKS + 2 * PARTS, k < PIECES - 1))
        def _():
            w_copy(2, 0, chunk_of(k) + 1).start()

        @pl.when(downs_1)
        def _():
            for tile in range(tiles):
                for which in range(2):
                    d_copy(which, 2 * part_of(k), tile, True).start()

        def backs(side, _):
            for which in range(2):
                serve(4 + 2 * side + which, (4 + which, 6 + which))

                @pl.when(gated)
                def _(which=which):
                    weight_part(side, which, k)

                @pl.when(downs_1)
                def _(which=which):
                    through_layer(which, k, side)

            return 0

        lax.fori_loop(0, 2, backs, 0)

        @pl.when(jnp.logical_and(gated, layer == 1))
        def _():
            for tile in range(tiles - 2, tiles):
                p_copy(k, tile).wait()
            for which in range(2):
                for tile in range(tiles):
                    d_copy(which, chunk_of(k), tile, False).wait()

        @pl.when(k == CHUNKS - 1)
        def _():
            x_copy.start()

        @pl.when(k == CHUNKS + PARTS - 1)
        def _():
            w_copy(2, 0, 0).start()
            through_norm()
            for tile in range(2):
                for which in range(2):
                    gu_copy(which, 0, tile).start()
            turn(dh, dht)
            x_copy.wait()
            norm_all()

        return 0

    lax.fori_loop(0, TICKS, tick, 0)


def train_step(x, dy, h, p0, gate, up, weights, ms, vs):
    tokens, d = dy.shape
    ff = p0.shape[1]
    c, r, e = ff // CHUNKS, d // 32, d // PARTS
    rows = min(512, tokens // 4)
    any_ = pl.BlockSpec(memory_space=pl.ANY)
    blocks = lambda *n: pltpu.VMEM((*n, GROUPS, r, e), BF)
    scratch = [
        pltpu.VMEM((tokens, d), BF), pltpu.VMEM((d, tokens), BF), pltpu.VMEM((tokens, d), BF), pltpu.VMEM((d, tokens), BF),
        pltpu.VMEM((d, c), BF), pltpu.VMEM((d, c), BF), pltpu.VMEM((c, d), BF),
        pltpu.VMEM((tokens, c), BF), pltpu.VMEM((tokens, c), BF),
        pltpu.VMEM((2, rows, c), BF),
        pltpu.VMEM((rows, 4 * c), F32),
        blocks(2, SUBS, 32), blocks(2, SUBS, 32),
        *[blocks(2, SUBS, 16 >> s) for s in range(STAGES)] * 2,
        *[blocks(SUBS, 16 >> s) for s in range(STAGES - 1)] * 2,
        blocks(2, SUBS), *[pltpu.VMEM((2, SUBS, GROUPS, r, e), F32)] * 2, blocks(2, SUBS),
        pltpu.SemaphoreType.DMA((2, STAGES, SUBS)), pltpu.SemaphoreType.DMA((2, STAGES, SUBS, 2)),
        pltpu.SemaphoreType.DMA((2, STAGES, SUBS)), pltpu.SemaphoreType.DMA((2, STAGES, SUBS, 2)),
        pltpu.SemaphoreType.DMA((2, SUBS)), pltpu.SemaphoreType.DMA((4,)), pltpu.SemaphoreType.DMA((3,)), pltpu.SemaphoreType.DMA((2,)),
        pltpu.SemaphoreType.DMA((2, 3, 4)), pltpu.SemaphoreType.DMA((2, 4)), pltpu.SemaphoreType.DMA((4,)),
    ]
    packed = jax.ShapeDtypeStruct((PIECES, SUBS, 32, GROUPS, r, e), BF)
    like = [jax.ShapeDtypeStruct(t.shape, F32) for t in (*ms, *vs)]
    return pl.pallas_call(
        step_kernel,
        name="step",
        in_specs=[any_] * 15,
        out_specs=[any_] * 11,
        out_shape=[packed, packed, *like, *[jax.ShapeDtypeStruct((tokens, ff), BF)] * 3],
        scratch_shapes=scratch,
        compiler_params=pltpu.CompilerParams(collective_id=0, has_side_effects=True, vmem_limit_bytes=67_000_000),
        cost_estimate=pl.CostEstimate(flops=28 * tokens * d * ff, bytes_accessed=400 << 20, transcendentals=0),
    )(x, dy, h, p0, gate, up, *weights, *ms, *vs)


def unpack_kernel(gate_ref, up_ref, down_a, down_b, *refs):
    r, e = gate_ref.shape[-2:]
    moments, (wg_ref, wu_ref, wd_ref), moments_out = refs[:6], refs[6:9], refs[9:]
    for source, to in zip(moments, moments_out, strict=True):
        to[...] = source[...]
    for core in range(2):
        for z0 in range(2):
            for z1 in range(2):
                owner = z1 * 4 + z0 * 2 + core
                for group in range(4):
                    sub, q = group // GROUPS, group % GROUPS
                    for chunk in range(CHUNKS):
                        at_rows, at_cols = pl.ds(owner * r, r), pl.ds((chunk * 4 + group) * e, e)
                        wg_ref[at_rows, at_cols] = gate_ref[chunk, sub, core, z0, z1, q]
                        wu_ref[at_rows, at_cols] = up_ref[chunk, sub, core, z0, z1, q]
                    for part in range(PARTS):
                        for half, ref in enumerate((down_a, down_b)):
                            at_rows = pl.ds((owner * 8 + half * 4 + group) * r, r)
                            wd_ref[at_rows, pl.ds(part * e, e)] = ref[part, sub, core, z0, z1, q]


def unpack(wa, wb, moments, d, ff):
    r, e = wa.shape[-2:]
    wa, wb = (t.reshape(PIECES, SUBS, *(2,) * 5, GROUPS, r, e) for t in (wa, wb))

    def spec(n, first, half):
        def index(layer, x, y):
            outer, inner = (x, y) if half == 0 else (y, x)
            return (first(layer), 0, 0, outer, 0, inner, 0, 0, 0, 0)

        return pl.BlockSpec((n, SUBS, 2, None, 2, None, 2, GROUPS, r, e), index)

    wide, part = lambda layer: 2 - 2 * layer, lambda layer: 3 - layer
    slab = lambda rows, cols: pl.BlockSpec((None, rows, cols), lambda layer, x, y: (layer, 2 * x + y, 0))
    moment = [
        pl.BlockSpec((None, r, ff // 4), lambda layer, x, y: (layer, 0, 2 * x + y)) if t.shape[2] == ff else slab(2 * r, d) for t in moments
    ]
    return pl.pallas_call(
        unpack_kernel,
        name="unpack",
        grid=(2, 2, 2),
        in_specs=[spec(CHUNKS, wide, 0), spec(CHUNKS, wide, 1), spec(PARTS, part, 0), spec(PARTS, part, 1), *moment],
        out_specs=[slab(d // 4, ff), slab(d // 4, ff), slab(ff // 4, d), *moment],
        out_shape=[jax.ShapeDtypeStruct((2, d, ff), BF)] * 2
        + [jax.ShapeDtypeStruct((2, ff, d), BF)]
        + [jax.ShapeDtypeStruct(t.shape, F32) for t in moments],
        compiler_params=pltpu.CompilerParams(vmem_limit_bytes=60 << 20),
    )(wa, wb, wa, wb, *moments)


def solution(mesh):
    def step(x, dy, *arrays):
        wg, wu, wd = arrays[:3]
        ms, vs = arrays[3:6], arrays[6:9]
        x, dy = x[0], dy[0]
        p0, h, gate, up = forward(x, wg, wu, wd, 0)
        wa, wb, *moments, _, _, _ = train_step(x, dy, h, p0, gate, up, (wg, wu, wd), ms, vs)
        return tuple(unpack(wa, wb, moments, x.shape[1], wg.shape[2]))

    seq, whole, rows = P(("rep", "dp")), P(), P(None, "dp")
    return jax.shard_map(
        step,
        mesh=mesh,
        in_specs=(seq, seq) + (whole,) * 3 + (rows,) * 6,
        out_specs=(P("rep"),) * 3 + (P("rep", "dp"),) * 6,
        check_vma=False,
    )
```

```python
import functools

import jax
import jax.numpy as jnp
from jax import lax
from jax.experimental import pallas as pl
from jax.experimental.pallas import tpu as pltpu
from jax.sharding import PartitionSpec as P

BF = jnp.bfloat16
F32 = jnp.float32
MESH = pl.DeviceIdType.MESH
NN, NT = ((1,), (0,)), ((1,), (1,))

CORE, Z0, Z1, Y, X = 1, 2, 4, 8, 16
ORDERS = ((CORE, X, Z0, Y, Z1), (CORE, Y, Z0, X, Z1))
STAGES = 5
CHUNKS = 6
PARTS = 3
PIECES = 2 * (CHUNKS + PARTS)
FRONT = 4
STRIP = 32
SUBS = 2
GROUPS = 4 // SUBS
POINTS = 8
TIMES = (
    (8, 9, 12, 17, 20, 24, 28, 30, 37, 41, 45),
    (9, 10, 14, 20, 22, 26, 29, 34, 39, 47, 51),
)
TICKS = PIECES + max(t[-1] for t in TIMES) // POINTS


def dot(a, b, dims=NN):
    return lax.dot_general(a, b, (dims, ((), ())), preferred_element_type=F32)


def bit_of(i, bit):
    return (i // bit) % 2


def place(i, order):
    at = 0
    for bit in order:
        at = at * 2 + bit_of(i, bit)
    return at


def sigmoid(x):
    return 1.0 / (1.0 + jnp.exp(-x))


def normed(h):
    wide = h.astype(F32)
    return (wide * lax.rsqrt(jnp.mean(wide**2, -1, keepdims=True) + 1e-6)).astype(BF)


def adamw(w, m, v, g):
    m = 0.9 * m + 0.1 * g
    v = 0.95 * v + 0.05 * g * g
    step = m * lax.rsqrt(v + 1e-8) + 0.1 * w
    return (w - 0.02 * step).astype(BF), m, v


def forward_kernel(x_ref, wg_ref, wu_ref, wd_ref, p_ref, h_ref, gate_ref, up_ref, a_all, total):
    chunk, tile = pl.program_id(0), pl.program_id(1)
    rows = p_ref.shape[0]
    here = pl.ds(pl.multiple_of(tile * rows, rows), rows)

    @pl.when(chunk == 0)
    def _():
        a_all[here, :] = normed(x_ref[...])

    a = a_all[here, :]
    gate, up = dot(a, wg_ref[...]), dot(a, wu_ref[...])
    gate_ref[...], up_ref[...] = gate, up
    p = (gate * sigmoid(gate) * up).astype(BF)
    p_ref[...] = p

    @pl.when(chunk == 0)
    def _():
        total[here, :] = dot(p, wd_ref[...])

    @pl.when(chunk > 0)
    def _():
        total[here, :] += dot(p, wd_ref[...])

    @pl.when(chunk == pl.num_programs(0) - 1)
    def _():
        down = total[here, :].astype(BF).astype(F32)
        h_ref[...] = (x_ref[...].astype(F32) + down).astype(BF)


def forward(x, wg, wu, wd, layer):
    tokens, d = x.shape
    ff = wg.shape[-1]
    c, rows = ff // CHUNKS, min(512, tokens // 4)
    last = tokens // rows - 1
    return pl.pallas_call(
        forward_kernel,
        name="forward",
        grid=(CHUNKS, tokens // rows),
        in_specs=[
            pl.BlockSpec((rows, d), lambda i, t: (jnp.where((i == 0) | (i == CHUNKS - 1), t, last), 0)),
            pl.BlockSpec((None, d, c), lambda i, t: (layer, 0, i)),
            pl.BlockSpec((None, d, c), lambda i, t: (layer, 0, i)),
            pl.BlockSpec((None, c, d), lambda i, t: (layer, i, 0)),
        ],
        out_specs=[
            pl.BlockSpec((rows, c), lambda i, t: (t, i)),
            pl.BlockSpec((rows, d), lambda i, t: (jnp.where(i == CHUNKS - 1, t, 0), 0)),
            *[pl.BlockSpec((None, rows, c), lambda i, t: (i, t, 0))] * 2,
        ],
        out_shape=[
            jax.ShapeDtypeStruct((tokens, ff), BF),
            jax.ShapeDtypeStruct((tokens, d), BF),
            *[jax.ShapeDtypeStruct((CHUNKS, tokens, c), F32)] * 2,
        ],
        scratch_shapes=[pltpu.VMEM((tokens, d), BF), pltpu.VMEM((tokens, d), F32)],
        compiler_params=pltpu.CompilerParams(vmem_limit_bytes=60 << 20),
        cost_estimate=pl.CostEstimate(flops=6 * tokens * d * ff, bytes_accessed=60 << 20, transcendentals=0),
    )(x, wg, wu, wd)


def step_kernel(
    x_hbm, dy_hbm, h_hbm, p0_hbm, gate_hbm, up_hbm, wg_hbm, wu_hbm, wd_hbm, mg_hbm, mu_hbm, md_hbm, vg_hbm, vu_hbm, vd_hbm,
    wa_out, wb_out, mg_out, mu_out, md_out, vg_out, vu_out, vd_out, p1_hbm, dg_hbm, du_hbm,
    a, at, dh, dht, wg, wu, wd, dg, du, ps, big, ga, gb, *rest,
):
    (ra, rb, sa, sb), rest = (rest[0:5], rest[5:10], rest[10:14], rest[14:18]), rest[18:]
    wn, mo, vo, wo, *rest = rest
    rs_send, rs_recv, ag_send, ag_recv, own_sem, load_sem, w_sem, p_sem, opt_sem, d_sem, gu_sem = rest

    tokens, d = a.shape
    c = wg.shape[1]
    r = d // 32
    e = d // PARTS
    rows = ps.shape[1]
    tiles = tokens // rows
    wide = 4 * 8 * r
    me = lax.axis_index("dp")
    g_bufs, r_bufs, s_bufs, w_outs = (ga, gb), (ra, rb), (sa, sb), (wa_out, wb_out)
    mine = [place(me, order) for order in ORDERS]

    barrier = pltpu.get_barrier_semaphore()
    for bit in (CORE, Z0, Z1, Y, X):
        other = me + bit * (1 - 2 * bit_of(me, bit))
        pl.semaphore_signal(barrier, inc=1, device_id={"dp": other}, device_id_type=MESH)
    pl.semaphore_wait(barrier, 5)

    def rs_copy(half, stage, piece, sub):
        bit = ORDERS[half][stage]
        own, n = bit_of(me, bit), 16 >> stage
        source = g_bufs[half].at[piece % 2, sub] if stage == 0 else s_bufs[half][stage - 1].at[sub]
        return pltpu.make_async_remote_copy(
            src_ref=source.at[pl.ds((1 - own) * n, n)],
            dst_ref=r_bufs[half][stage].at[piece % 2, sub],
            send_sem=rs_send.at[half, stage, sub],
            recv_sem=rs_recv.at[half, stage, sub, piece % 2],
            device_id={"dp": me + bit * (1 - 2 * own)},
            device_id_type=MESH,
        )

    def rs_start(stage, piece, sub):
        for half in range(2):
            rs_copy(half, stage, piece, sub).start()

    def rs_wait(stage, piece, sub):
        for half in range(2):
            copy = rs_copy(half, stage, piece, sub)
            copy.wait_send()
            copy.wait_recv()

    def rs_add(stage, piece, sub):
        n = 16 >> stage
        some = min(n, SUBS)
        for half in range(2):
            own = bit_of(me, ORDERS[half][stage])
            source = g_bufs[half].at[piece % 2, sub] if stage == 0 else s_bufs[half][stage - 1].at[sub]
            got, to = r_bufs[half][stage].at[piece % 2, sub], s_bufs[half][stage].at[sub]

            def add(i, _, source=source, got=got, to=to, own=own):
                here = pl.ds(i * some, some)
                to[here] = (source[pl.ds(own * n + i * some, some)].astype(F32) + got[here].astype(F32)).astype(BF)
                return 0

            lax.fori_loop(0, n // some, add, 0)

    def rs_sum(half, piece, sub):
        stage = STAGES - 1
        own = bit_of(me, ORDERS[half][stage])
        total = s_bufs[half][stage - 1][sub, own].astype(F32) + r_bufs[half][stage][piece % 2, sub, 0].astype(F32)
        return total.astype(BF).astype(F32)

    def ag_copy(half, stage, piece, sub):
        bit = ORDERS[half][STAGES - 1 - stage]
        n = 1 << stage
        if stage == 0:
            source, to = wn.at[half, sub], w_outs[half].at[piece, sub, mine[half]]
        else:
            source = to = w_outs[half].at[piece, sub, pl.ds((mine[half] // n) * n, n)]
        return pltpu.make_async_remote_copy(
            src_ref=source,
            dst_ref=to,
            send_sem=ag_send.at[half, stage, sub],
            recv_sem=ag_recv.at[half, stage, sub, piece % 2],
            device_id={"dp": me + bit * (1 - 2 * bit_of(me, bit))},
            device_id_type=MESH,
        )

    def own_copy(half, piece, sub):
        return pltpu.make_async_copy(wn.at[half, sub], w_outs[half].at[piece, sub, mine[half]], own_sem.at[half, sub])

    def ag_start(stage, piece, sub):
        for half in range(2):
            ag_copy(half, stage, piece, sub).start()
            if stage == 0:
                own_copy(half, piece, sub).start()

    def ag_finish(stage, piece, sub):
        for half in range(2):
            copy = ag_copy(half, stage, piece, sub)
            copy.wait_send()
            copy.wait_recv()
            if stage == 0:
                own_copy(half, piece, sub).wait()

    def is_wide(piece):
        return jnp.logical_or(piece < CHUNKS, piece >= CHUNKS + 2 * PARTS)

    def layer_of(piece):
        return jnp.where(piece < CHUNKS + PARTS, 1, 0)

    def chunk_of(piece):
        return jnp.where(piece < CHUNKS, piece, piece - CHUNKS - 2 * PARTS)

    def part_of(piece):
        return jnp.where(piece < CHUNKS + PARTS, piece - CHUNKS, piece - CHUNKS - PARTS)

    def opt_do(piece, sub, out, start):
        layer = layer_of(piece)
        part_cols = pl.ds(pl.multiple_of(part_of(piece) * e, e), e)

        def copies(wide):
            for half in range(2):
                for q in range(GROUPS):
                    group = sub * GROUPS + q
                    wide_cols = pl.ds(pl.multiple_of(chunk_of(piece) * c + group * e, e), e)
                    row = (half * 4 + group) * r
                    rows_, cols = (slice(None), wide_cols) if wide else (pl.ds(row, r), part_cols)
                    if wide:
                        kinds = ((mg_hbm, mu_hbm)[half], (mg_out, mu_out)[half], mo), ((vg_hbm, vu_hbm)[half], (vg_out, vu_out)[half], vo)
                    else:
                        kinds = (md_hbm, md_out, mo), (vd_hbm, vd_out, vo)
                    for k, (hbm, hbm_out, vmem) in enumerate(kinds):
                        sem = opt_sem.at[half, k, group]
                        if out:
                            yield pltpu.make_async_copy(vmem.at[half, sub, q], hbm_out.at[layer, rows_, cols], sem)
                        else:
                            yield pltpu.make_async_copy(hbm.at[layer, rows_, cols], vmem.at[half, sub, q], sem)
                    if not out:
                        own = pl.ds(pl.multiple_of(me * r if wide else me * 8 * r + row, 8), r)
                        source = (wg_hbm, wu_hbm)[half] if wide else wd_hbm
                        yield pltpu.make_async_copy(source.at[layer, own, cols], wo.at[half, sub, q], opt_sem.at[half, 2, group])

        if not start:
            for half in range(2):
                for q in range(GROUPS):
                    for k, vmem in enumerate((mo, vo, wo)[: 2 if out else 3]):
                        block = (mg_hbm, vg_hbm, wg_hbm)[k].at[0, pl.ds(0, r), pl.ds(0, e)]
                        pltpu.make_async_copy(block, vmem.at[half, sub, q], opt_sem.at[half, k, sub * GROUPS + q]).wait()
            return
        for wide in (True, False):

            @pl.when(is_wide(piece) == wide)
            def _(wide=wide):
                for copy in copies(wide):
                    copy.start()

    def opt_step(piece, sub):
        for half in range(2):
            w, m, v = adamw(wo[half, sub].astype(F32), mo[half, sub], vo[half, sub], rs_sum(half, piece, sub))
            wn[half, sub], mo[half, sub], vo[half, sub] = w, m, v

    def go_on(event, piece, sub):
        if event < STAGES:
            if event >= 0:
                rs_wait(event, piece, sub)
            if 0 <= event < STAGES - 1:
                rs_add(event, piece, sub)
            if event < STAGES - 1:
                rs_start(event + 1, piece, sub)
            if event == STAGES - 2:
                opt_do(piece, sub, False, True)
            if event == STAGES - 1:
                opt_do(piece, sub, False, False)
                opt_step(piece, sub)
                opt_do(piece, sub, True, True)
                ag_start(0, piece, sub)
        else:
            ag_finish(event - STAGES, piece, sub)
            if event == STAGES:
                opt_do(piece, sub, True, False)
            if event < 2 * STAGES - 1:
                ag_start(event - STAGES + 1, piece, sub)

    def service(k, point):
        due = [(event - 1, sub, at) for sub in range(SUBS) for event, at in enumerate(TIMES[sub]) if at % POINTS == point]
        for event, sub, at in sorted(due, key=lambda one: (-one[0], -one[2], one[1])):
            piece = k - at // POINTS

            @pl.when(jnp.logical_and(piece >= 0, piece < PIECES))
            def _(event=event, piece=piece, sub=sub):
                go_on(event, piece, sub)

    def w_copy(which, layer, chunk):
        at_cols = pl.ds(pl.multiple_of(chunk * c, c), c)
        if which == 2:
            return pltpu.make_async_copy(wd_hbm.at[layer, at_cols, :], wd, w_sem.at[2])
        return pltpu.make_async_copy((wg_hbm, wu_hbm)[which].at[layer, :, at_cols], (wg, wu)[which], w_sem.at[which])

    def p_copy(piece, tile):
        slot = tile % 2
        at_cols = pl.ds(pl.multiple_of(chunk_of(piece) * c, c), c)
        return pltpu.make_async_copy(ps.at[slot], p1_hbm.at[pl.ds(pl.multiple_of(tile * rows, rows), rows), at_cols], p_sem.at[slot])

    def d_copy(which, chunk, tile, load):
        here = pl.ds(pl.multiple_of(tile * rows, rows), rows)
        vmem, hbm = (dg, du)[which].at[here, :], (dg_hbm, du_hbm)[which].at[chunk, here, :]
        return pltpu.make_async_copy(*((hbm, vmem) if load else (vmem, hbm)), d_sem.at[which, tile])

    def front_tile(piece, tile):
        here = pl.ds(pl.multiple_of(tile * rows, rows), rows)
        at_, dh_ = a[here, :], dh[here, :]

        @pl.when(tile >= 2)
        def _():
            p_copy(piece, tile - 2).wait()

        n = c // FRONT
        for j in range(FRONT):
            cols = slice(j * n, (j + 1) * n)
            gates, ups = dot(at_, wg[:, cols]), dot(at_, wu[:, cols])
            dps = dot(dh_, wd[cols, :], NT)
            for i in range(0, rows, STRIP):
                gate, up = gates[i : i + STRIP], ups[i : i + STRIP]
                dp = dps[i : i + STRIP].astype(BF).astype(F32)
                s = sigmoid(gate)
                gs = gate * s
                out = pl.ds(pl.multiple_of(tile * rows + i, STRIP), STRIP)
                ps[tile % 2, i : i + STRIP, cols] = (gs * up).astype(BF)
                du[out, cols] = (dp * gs).astype(BF)
                dg[out, cols] = (dp * up * (s + gs * (1.0 - s))).astype(BF)

        p_copy(piece, tile).start()
        for which in range(2):
            d_copy(which, chunk_of(piece), tile, False).start()

    def gu_copy(which, chunk, tile):
        slot = 2 * (tile % 2) + which
        source = (gate_hbm, up_hbm)[which].at[chunk, pl.ds(pl.multiple_of(tile * rows, rows), rows), :]
        return pltpu.make_async_copy(source, big.at[slot], gu_sem.at[slot])

    def kept_tile(piece, tile):
        here = pl.ds(pl.multiple_of(tile * rows, rows), rows)
        dh_ = dh[here, :]
        for which in range(2):
            gu_copy(which, chunk_of(piece), tile).wait()
        n = c // FRONT
        for j in range(FRONT):
            cols = slice(j * n, (j + 1) * n)
            dps = dot(dh_, wd[cols, :], NT)
            slot = 2 * (tile % 2)
            for i in range(0, rows, STRIP):
                gate, up = big[slot, i : i + STRIP, cols], big[slot + 1, i : i + STRIP, cols]
                dp = dps[i : i + STRIP].astype(BF).astype(F32)
                s = sigmoid(gate)
                gs = gate * s
                out = pl.ds(pl.multiple_of(tile * rows + i, STRIP), STRIP)
                du[out, cols] = (dp * gs).astype(BF)
                dg[out, cols] = (dp * up * (s + gs * (1.0 - s))).astype(BF)

        following = piece * tiles + tile + 2

        @pl.when(following < PIECES * tiles)
        def _():
            for which in range(2):
                gu_copy(which, following // tiles - CHUNKS - 2 * PARTS, following % tiles).start()

    def weight_part(side, which, piece):
        n = c // 2
        term = dot(at[...], (dg, du)[which][:, pl.ds(pl.multiple_of(side * n, n), n)])
        for i in range(32):
            for q in range(2):
                group = side * 2 + q
                block = term[i * r : (i + 1) * r, q * e : (q + 1) * e].astype(BF)
                (ga, gb)[which][piece % 2, group // GROUPS, place(i, ORDERS[which]), group % GROUPS] = block

    def through_layer(which, piece, side):
        chunk = 2 * part_of(piece) + side
        w_copy(which, 1, chunk).wait()

        def back(tile, _):
            here = pl.ds(pl.multiple_of(tile * rows, rows), rows)
            total = pl.ds(0, d)
            d_copy(which, chunk, tile, True).wait()
            part = dot((dg, du)[which][here, :], (wg, wu)[which][...], NT)
            if which == 0:
                big[tile, :, total] = jnp.where(chunk == 0, jnp.zeros_like(part), big[tile, :, total]) + part
            else:
                big[tile, :, total] += part

            @pl.when(side == 0)
            def _():
                d_copy(which, chunk + 1, tile, True).start()

            return 0

        lax.fori_loop(0, tiles, back, 0)

        @pl.when(side == 0)
        def _():
            w_copy(which, 1, chunk + 1).start()

    def tile_copy(which, tile, source):
        from_cols = pl.ds(pl.multiple_of(tile * wide, 128), wide)
        return pltpu.make_async_copy(source.at[:, from_cols], (dg, du)[which].at[:, pl.ds(0, wide)], load_sem.at[which])

    def tile_start(piece, which, tile):
        for layer, source in enumerate((p0_hbm, p1_hbm)):

            @pl.when(layer_of(piece) == layer)
            def _(source=source):
                tile_copy(which, tile, source).start()

    def down_tile(piece, which, tile):
        tile_copy(which, tile, p0_hbm).wait()
        at_rows = pl.ds(pl.multiple_of(part_of(piece) * e, e), e)
        term = dot(dht[at_rows, :], (dg, du)[which][:, :wide]).T
        for i in range(4):
            for j in range(8):
                half, group = j // 4, j % 4
                block = term[(8 * i + j) * r : (8 * i + j + 1) * r, :].astype(BF)
                g_bufs[half][piece % 2, group // GROUPS, place(4 * tile + i, ORDERS[half]), group % GROUPS] = block

        @pl.when(tile + 2 < 8)
        def _():
            tile_start(piece, which, tile + 2)

    def h_copy(tile):
        slot, here = tile % 2, pl.ds(pl.multiple_of(tile * rows, rows), rows)
        return pltpu.make_async_copy(h_hbm.at[here, :], ps.at[slot, :, pl.ds(0, d)], p_sem.at[slot])

    def through_norm():
        def back(tile, _):
            h_copy(tile).wait()

            def some(i, _):
                at_rows = pl.ds(pl.multiple_of(i * 32, 32), 32)
                at_all = pl.ds(pl.multiple_of(tile * rows + i * 32, 32), 32)
                h = ps[tile % 2, at_rows, pl.ds(0, d)].astype(F32)
                by_a = big[tile, at_rows, pl.ds(0, d)].astype(BF).astype(F32)
                scale = lax.rsqrt(jnp.mean(h * h, -1, keepdims=True) + 1e-6)
                along = jnp.sum(by_a * h, -1, keepdims=True)
                by_h = (by_a * scale - h * (scale * scale * scale * along * (1.0 / d))).astype(BF)
                dh[at_all, :] = (dh[at_all, :].astype(F32) + by_h.astype(F32)).astype(BF)
                return 0

            lax.fori_loop(0, rows // 32, some, 0)

            @pl.when(tile + 2 < tiles)
            def _():
                h_copy(tile + 2).start()

            return 0

        lax.fori_loop(0, tiles, back, 0)

    def turn(source, to):
        def back(tile, _):
            here = pl.ds(pl.multiple_of(tile * rows, rows), rows)
            to[:, here] = source[here, :].astype(F32).T.astype(BF)
            return 0

        lax.fori_loop(0, tiles, back, 0)

    def norm_all():
        def back(i, _):
            here = pl.ds(pl.multiple_of(i * 32, 32), 32)
            a[here, :] = normed(a[here, :])
            return 0

        lax.fori_loop(0, tokens // 32, back, 0)
        turn(a, at)

    first = (
        pltpu.make_async_copy(h_hbm, a, load_sem.at[2]),
        pltpu.make_async_copy(dy_hbm, dh, load_sem.at[3]),
        *(w_copy(which, 1, 0) for which in range(3)),
    )
    for copy in first:
        copy.start()
    first[0].wait()
    norm_all()
    first[1].wait()
    turn(dh, dht)
    x_copy = pltpu.make_async_copy(x_hbm, a, load_sem.at[2])

    def tick(k, _):
        computes = k < PIECES
        layer = layer_of(k)
        gated = jnp.logical_and(computes, is_wide(k))
        downs = jnp.logical_and(computes, jnp.logical_not(is_wide(k)))
        downs_1 = jnp.logical_and(downs, layer == 1)

        @pl.when(downs)
        def _():
            tile_start(k, 0, 0)
            tile_start(k, 1, 1)

        @pl.when(downs_1)
        def _():
            for which in range(2):
                w_copy(which, 1, 2 * part_of(k)).start()

        def serve(point, points):
            for one in points:

                @pl.when(point == one)
                def _(one=one):
                    service(k, one)

        def fronts(point, _):
            serve(point, range(4))

            @pl.when(jnp.logical_and(gated, layer == 1))
            def _():
                @pl.when(point == 0)
                def _():
                    for which in range(3):
                        w_copy(which, 1, chunk_of(k)).wait()

                front_tile(k, point)

            @pl.when(jnp.logical_and(gated, layer == 0))
            def _():
                @pl.when(point == 0)
                def _():
                    w_copy(2, 0, chunk_of(k)).wait()

                kept_tile(k, point)

            @pl.when(downs)
            def _():
                for which in range(2):
                    down_tile(k, which, 2 * point + which)

            return 0

        lax.fori_loop(0, 4, fronts, 0)

        @pl.when(k < CHUNKS - 1)
        def _():
            for which in range(3):
                w_copy(which, 1, chunk_of(k) + 1).start()

        @pl.when(jnp.logical_and(k >= CHUNKS + 2 * PARTS, k < PIECES - 1))
        def _():
            w_copy(2, 0, chunk_of(k) + 1).start()

        @pl.when(downs_1)
        def _():
            for tile in range(tiles):
                for which in range(2):
                    d_copy(which, 2 * part_of(k), tile, True).start()

        def backs(side, _):
            for which in range(2):
                serve(4 + 2 * side + which, (4 + which, 6 + which))

                @pl.when(gated)
                def _(which=which):
                    weight_part(side, which, k)

                @pl.when(downs_1)
                def _(which=which):
                    through_layer(which, k, side)

            return 0

        lax.fori_loop(0, 2, backs, 0)

        @pl.when(jnp.logical_and(gated, layer == 1))
        def _():
            for tile in range(tiles - 2, tiles):
                p_copy(k, tile).wait()
            for which in range(2):
                for tile in range(tiles):
                    d_copy(which, chunk_of(k), tile, False).wait()

        @pl.when(k == CHUNKS - 1)
        def _():
            x_copy.start()
            for tile in range(2):
                h_copy(tile).start()

        @pl.when(k == CHUNKS + PARTS - 1)
        def _():
            w_copy(2, 0, 0).start()
            through_norm()
            for tile in range(2):
                for which in range(2):
                    gu_copy(which, 0, tile).start()
            turn(dh, dht)

        @pl.when(k == CHUNKS + PARTS)
        def _():
            x_copy.wait()
            norm_all()

        return 0

    lax.fori_loop(0, TICKS, tick, 0)


def train_step(x, dy, h, p0, gate, up, weights, ms, vs):
    tokens, d = dy.shape
    ff = p0.shape[1]
    c, r, e = ff // CHUNKS, d // 32, d // PARTS
    rows = min(512, tokens // 4)
    any_ = pl.BlockSpec(memory_space=pl.ANY)
    blocks = lambda *n: pltpu.VMEM((*n, GROUPS, r, e), BF)
    scratch = [
        pltpu.VMEM((tokens, d), BF), pltpu.VMEM((d, tokens), BF), pltpu.VMEM((tokens, d), BF), pltpu.VMEM((d, tokens), BF),
        pltpu.VMEM((d, c), BF), pltpu.VMEM((d, c), BF), pltpu.VMEM((c, d), BF),
        pltpu.VMEM((tokens, c), BF), pltpu.VMEM((tokens, c), BF),
        pltpu.VMEM((2, rows, c), BF),
        pltpu.VMEM((4, rows, c), F32),
        blocks(2, SUBS, 32), blocks(2, SUBS, 32),
        *[blocks(2, SUBS, 16 >> s) for s in range(STAGES)] * 2,
        *[blocks(SUBS, 16 >> s) for s in range(STAGES - 1)] * 2,
        blocks(2, SUBS), *[pltpu.VMEM((2, SUBS, GROUPS, r, e), F32)] * 2, blocks(2, SUBS),
        pltpu.SemaphoreType.DMA((2, STAGES, SUBS)), pltpu.SemaphoreType.DMA((2, STAGES, SUBS, 2)),
        pltpu.SemaphoreType.DMA((2, STAGES, SUBS)), pltpu.SemaphoreType.DMA((2, STAGES, SUBS, 2)),
        pltpu.SemaphoreType.DMA((2, SUBS)), pltpu.SemaphoreType.DMA((4,)), pltpu.SemaphoreType.DMA((3,)), pltpu.SemaphoreType.DMA((2,)),
        pltpu.SemaphoreType.DMA((2, 3, 4)), pltpu.SemaphoreType.DMA((2, 4)), pltpu.SemaphoreType.DMA((4,)),
    ]
    packed = jax.ShapeDtypeStruct((PIECES, SUBS, 32, GROUPS, r, e), BF)
    like = [jax.ShapeDtypeStruct(t.shape, F32) for t in (*ms, *vs)]
    return pl.pallas_call(
        step_kernel,
        name="step",
        in_specs=[any_] * 15,
        out_specs=[any_] * 11,
        out_shape=[packed, packed, *like, jax.ShapeDtypeStruct((tokens, ff), BF), *[jax.ShapeDtypeStruct((CHUNKS, tokens, c), BF)] * 2],
        scratch_shapes=scratch,
        compiler_params=pltpu.CompilerParams(collective_id=0, has_side_effects=True, vmem_limit_bytes=67_000_000),
        cost_estimate=pl.CostEstimate(flops=28 * tokens * d * ff, bytes_accessed=400 << 20, transcendentals=0),
    )(x, dy, h, p0, gate, up, *weights, *ms, *vs)


def unpack_kernel(gate_ref, up_ref, down_a, down_b, *refs):
    r, e = gate_ref.shape[-2:]
    moments, (wg_ref, wu_ref, wd_ref), moments_out = refs[:6], refs[6:9], refs[9:]
    for source, to in zip(moments, moments_out, strict=True):
        to[...] = source[...]
    for core in range(2):
        for z0 in range(2):
            for z1 in range(2):
                owner = z1 * 4 + z0 * 2 + core
                for group in range(4):
                    sub, q = group // GROUPS, group % GROUPS
                    for chunk in range(CHUNKS):
                        at_rows, at_cols = pl.ds(owner * r, r), pl.ds((chunk * 4 + group) * e, e)
                        wg_ref[at_rows, at_cols] = gate_ref[chunk, sub, core, z0, z1, q]
                        wu_ref[at_rows, at_cols] = up_ref[chunk, sub, core, z0, z1, q]
                    for part in range(PARTS):
                        for half, ref in enumerate((down_a, down_b)):
                            at_rows = pl.ds((owner * 8 + half * 4 + group) * r, r)
                            wd_ref[at_rows, pl.ds(part * e, e)] = ref[part, sub, core, z0, z1, q]


def unpack(wa, wb, moments, d, ff):
    r, e = wa.shape[-2:]
    wa, wb = (t.reshape(PIECES, SUBS, *(2,) * 5, GROUPS, r, e) for t in (wa, wb))

    def spec(n, first, half):
        def index(layer, x, y):
            outer, inner = (x, y) if half == 0 else (y, x)
            return (first(layer), 0, 0, outer, 0, inner, 0, 0, 0, 0)

        return pl.BlockSpec((n, SUBS, 2, None, 2, None, 2, GROUPS, r, e), index)

    wide, part = lambda layer: 2 - 2 * layer, lambda layer: 3 - layer
    slab = lambda rows, cols: pl.BlockSpec((None, rows, cols), lambda layer, x, y: (layer, 2 * x + y, 0))
    moment = [
        pl.BlockSpec((None, r, ff // 4), lambda layer, x, y: (layer, 0, 2 * x + y)) if t.shape[2] == ff else slab(2 * r, d) for t in moments
    ]
    return pl.pallas_call(
        unpack_kernel,
        name="unpack",
        grid=(2, 2, 2),
        in_specs=[spec(CHUNKS, wide, 0), spec(CHUNKS, wide, 1), spec(PARTS, part, 0), spec(PARTS, part, 1), *moment],
        out_specs=[slab(d // 4, ff), slab(d // 4, ff), slab(ff // 4, d), *moment],
        out_shape=[jax.ShapeDtypeStruct((2, d, ff), BF)] * 2
        + [jax.ShapeDtypeStruct((2, ff, d), BF)]
        + [jax.ShapeDtypeStruct(t.shape, F32) for t in moments],
        compiler_params=pltpu.CompilerParams(vmem_limit_bytes=60 << 20),
    )(wa, wb, wa, wb, *moments)


def solution(mesh):
    def step(x, dy, *arrays):
        wg, wu, wd = arrays[:3]
        ms, vs = arrays[3:6], arrays[6:9]
        x, dy = x[0], dy[0]
        p0, h, gate, up = forward(x, wg, wu, wd, 0)
        wa, wb, *moments, _, _, _ = train_step(x, dy, h, p0, gate, up, (wg, wu, wd), ms, vs)
        return tuple(unpack(wa, wb, moments, x.shape[1], wg.shape[2]))

    seq, whole, rows = P(("rep", "dp")), P(), P(None, "dp")
    return jax.shard_map(
        step,
        mesh=mesh,
        in_specs=(seq, seq) + (whole,) * 3 + (rows,) * 6,
        out_specs=(P("rep"),) * 3 + (P("rep", "dp"),) * 6,
        check_vma=False,
    )
```

```python
import functools

import jax
import jax.numpy as jnp
from jax import lax
from jax.experimental import pallas as pl
from jax.experimental.pallas import tpu as pltpu
from jax.sharding import PartitionSpec as P

BF = jnp.bfloat16
F32 = jnp.float32
MESH = pl.DeviceIdType.MESH
NN, NT = ((1,), (0,)), ((1,), (1,))

CORE, Z0, Z1, Y, X = 1, 2, 4, 8, 16
ORDERS = ((CORE, X, Z0, Y, Z1), (CORE, Y, Z0, X, Z1))
STAGES = 5
CHUNKS = 6
PARTS = 3
PIECES = 2 * (CHUNKS + PARTS)
FRONT = 4
STRIP = 128
SUBS = 2
GROUPS = 4 // SUBS
SLOTS = 4
POINTS = 8
TIMES = (
    (8, 9, 13, 17, 21, 24, 28, 31, 38, 42, 45),
    (10, 11, 16, 21, 23, 27, 31, 35, 40, 48, 53),
)
TICKS = PIECES + max(t[-1] for t in TIMES) // POINTS


def dot(a, b, dims=NN):
    return lax.dot_general(a, b, (dims, ((), ())), preferred_element_type=F32)


def bit_of(i, bit):
    return (i // bit) % 2


def place(i, order):
    at = 0
    for bit in order:
        at = at * 2 + bit_of(i, bit)
    return at


def sigmoid(x):
    return 1.0 / (1.0 + jnp.exp(-x))


def normed(h):
    wide = h.astype(F32)
    return (wide * lax.rsqrt(jnp.mean(wide**2, -1, keepdims=True) + 1e-6)).astype(BF)


def adamw(w, m, v, g):
    m = 0.9 * m + 0.1 * g
    v = 0.95 * v + 0.05 * g * g
    step = m * lax.rsqrt(v + 1e-8) + 0.1 * w
    return (w - 0.02 * step).astype(BF), m, v


def forward_kernel(x_ref, wg_ref, wu_ref, wd_ref, p_ref, h_ref, gate_ref, up_ref, a_all, total):
    chunk, tile = pl.program_id(0), pl.program_id(1)
    rows = p_ref.shape[0]
    here = pl.ds(pl.multiple_of(tile * rows, rows), rows)

    @pl.when(chunk == 0)
    def _():
        a_all[here, :] = normed(x_ref[...])

    a = a_all[here, :]
    gate, up = dot(a, wg_ref[...]), dot(a, wu_ref[...])
    gate_ref[...], up_ref[...] = gate, up
    p = (gate * sigmoid(gate) * up).astype(BF)
    p_ref[...] = p

    @pl.when(chunk == 0)
    def _():
        total[here, :] = dot(p, wd_ref[...])

    @pl.when(chunk > 0)
    def _():
        total[here, :] += dot(p, wd_ref[...])

    @pl.when(chunk == pl.num_programs(0) - 1)
    def _():
        down = total[here, :].astype(BF).astype(F32)
        h_ref[...] = (x_ref[...].astype(F32) + down).astype(BF)


def forward(x, wg, wu, wd, layer):
    tokens, d = x.shape
    ff = wg.shape[-1]
    c, rows = ff // CHUNKS, min(512, tokens // 4)
    last = tokens // rows - 1
    return pl.pallas_call(
        forward_kernel,
        name="forward",
        grid=(CHUNKS, tokens // rows),
        in_specs=[
            pl.BlockSpec((rows, d), lambda i, t: (jnp.where((i == 0) | (i == CHUNKS - 1), t, last), 0)),
            pl.BlockSpec((None, d, c), lambda i, t: (layer, 0, i)),
            pl.BlockSpec((None, d, c), lambda i, t: (layer, 0, i)),
            pl.BlockSpec((None, c, d), lambda i, t: (layer, i, 0)),
        ],
        out_specs=[
            pl.BlockSpec((rows, c), lambda i, t: (t, i)),
            pl.BlockSpec((rows, d), lambda i, t: (jnp.where(i == CHUNKS - 1, t, 0), 0)),
            *[pl.BlockSpec((None, rows, c), lambda i, t: (i, t, 0))] * 2,
        ],
        out_shape=[
            jax.ShapeDtypeStruct((tokens, ff), BF),
            jax.ShapeDtypeStruct((tokens, d), BF),
            *[jax.ShapeDtypeStruct((CHUNKS, tokens, c), F32)] * 2,
        ],
        scratch_shapes=[pltpu.VMEM((tokens, d), BF), pltpu.VMEM((tokens, d), F32)],
        compiler_params=pltpu.CompilerParams(vmem_limit_bytes=60 << 20),
        cost_estimate=pl.CostEstimate(flops=6 * tokens * d * ff, bytes_accessed=60 << 20, transcendentals=0),
    )(x, wg, wu, wd)


def step_kernel(
    x_hbm, dy_hbm, h_hbm, p0_hbm, gate_hbm, up_hbm, wg_hbm, wu_hbm, wd_hbm, mg_hbm, mu_hbm, md_hbm, vg_hbm, vu_hbm, vd_hbm,
    wa_out, wb_out, mg_out, mu_out, md_out, vg_out, vu_out, vd_out, p1_hbm, dg_hbm, du_hbm,
    a, at, dh, dht, wg, wu, wd, dg, du, ps, big, ga, gb, *rest,
):
    (ra, rb, sa, sb), rest = (rest[0:5], rest[5:10], rest[10:14], rest[14:18]), rest[18:]
    wn, mo, vo, wo, *rest = rest
    rs_send, rs_recv, ag_send, ag_recv, own_sem, load_sem, w_sem, p_sem, opt_sem, d_sem, gu_sem = rest

    tokens, d = a.shape
    c = wg.shape[1]
    r = d // 32
    e = d // PARTS
    rows = ps.shape[1]
    tiles = tokens // rows
    wide = 4 * 8 * r
    me = lax.axis_index("dp")
    g_bufs, r_bufs, s_bufs, w_outs = (ga, gb), (ra, rb), (sa, sb), (wa_out, wb_out)
    mine = [place(me, order) for order in ORDERS]

    barrier = pltpu.get_barrier_semaphore()
    for bit in (CORE, Z0, Z1, Y, X):
        other = me + bit * (1 - 2 * bit_of(me, bit))
        pl.semaphore_signal(barrier, inc=1, device_id={"dp": other}, device_id_type=MESH)
    pl.semaphore_wait(barrier, 5)

    def rs_copy(half, stage, piece, sub):
        bit = ORDERS[half][stage]
        own, n = bit_of(me, bit), 16 >> stage
        source = g_bufs[half].at[piece % SLOTS, sub] if stage == 0 else s_bufs[half][stage - 1].at[sub]
        return pltpu.make_async_remote_copy(
            src_ref=source.at[pl.ds((1 - own) * n, n)],
            dst_ref=r_bufs[half][stage].at[piece % 2, sub],
            send_sem=rs_send.at[half, stage, sub],
            recv_sem=rs_recv.at[half, stage, sub, piece % 2],
            device_id={"dp": me + bit * (1 - 2 * own)},
            device_id_type=MESH,
        )

    def rs_start(stage, piece, sub):
        for half in range(2):
            rs_copy(half, stage, piece, sub).start()

    def rs_wait(stage, piece, sub):
        for half in range(2):
            copy = rs_copy(half, stage, piece, sub)
            copy.wait_send()
            copy.wait_recv()

    def rs_add(stage, piece, sub):
        n = 16 >> stage
        some = min(n, SUBS)
        for half in range(2):
            own = bit_of(me, ORDERS[half][stage])
            source = g_bufs[half].at[piece % SLOTS, sub] if stage == 0 else s_bufs[half][stage - 1].at[sub]
            got, to = r_bufs[half][stage].at[piece % 2, sub], s_bufs[half][stage].at[sub]

            def add(i, _, source=source, got=got, to=to, own=own):
                here = pl.ds(i * some, some)
                to[here] = (source[pl.ds(own * n + i * some, some)].astype(F32) + got[here].astype(F32)).astype(BF)
                return 0

            lax.fori_loop(0, n // some, add, 0)

    def rs_sum(half, piece, sub):
        stage = STAGES - 1
        own = bit_of(me, ORDERS[half][stage])
        total = s_bufs[half][stage - 1][sub, own].astype(F32) + r_bufs[half][stage][piece % 2, sub, 0].astype(F32)
        return total.astype(BF).astype(F32)

    def ag_copy(half, stage, piece, sub):
        bit = ORDERS[half][STAGES - 1 - stage]
        n = 1 << stage
        if stage == 0:
            source, to = wn.at[half, sub], w_outs[half].at[piece, sub, mine[half]]
        else:
            source = to = w_outs[half].at[piece, sub, pl.ds((mine[half] // n) * n, n)]
        return pltpu.make_async_remote_copy(
            src_ref=source,
            dst_ref=to,
            send_sem=ag_send.at[half, stage, sub],
            recv_sem=ag_recv.at[half, stage, sub, piece % 2],
            device_id={"dp": me + bit * (1 - 2 * bit_of(me, bit))},
            device_id_type=MESH,
        )

    def own_copy(half, piece, sub):
        return pltpu.make_async_copy(wn.at[half, sub], w_outs[half].at[piece, sub, mine[half]], own_sem.at[half, sub])

    def ag_start(stage, piece, sub):
        for half in range(2):
            ag_copy(half, stage, piece, sub).start()
            if stage == 0:
                own_copy(half, piece, sub).start()

    def ag_finish(stage, piece, sub):
        for half in range(2):
            copy = ag_copy(half, stage, piece, sub)
            copy.wait_send()
            copy.wait_recv()
            if stage == 0:
                own_copy(half, piece, sub).wait()

    def is_wide(piece):
        return jnp.logical_or(piece < CHUNKS, piece >= CHUNKS + 2 * PARTS)

    def layer_of(piece):
        return jnp.where(piece < CHUNKS + PARTS, 1, 0)

    def chunk_of(piece):
        return jnp.where(piece < CHUNKS, piece, piece - CHUNKS - 2 * PARTS)

    def part_of(piece):
        return jnp.where(piece < CHUNKS + PARTS, piece - CHUNKS, piece - CHUNKS - PARTS)

    def opt_do(piece, sub, out, start):
        layer = layer_of(piece)
        part_cols = pl.ds(pl.multiple_of(part_of(piece) * e, e), e)

        def copies(wide):
            for half in range(2):
                for q in range(GROUPS):
                    group = sub * GROUPS + q
                    wide_cols = pl.ds(pl.multiple_of(chunk_of(piece) * c + group * e, e), e)
                    row = (half * 4 + group) * r
                    rows_, cols = (slice(None), wide_cols) if wide else (pl.ds(row, r), part_cols)
                    if wide:
                        kinds = ((mg_hbm, mu_hbm)[half], (mg_out, mu_out)[half], mo), ((vg_hbm, vu_hbm)[half], (vg_out, vu_out)[half], vo)
                    else:
                        kinds = (md_hbm, md_out, mo), (vd_hbm, vd_out, vo)
                    for k, (hbm, hbm_out, vmem) in enumerate(kinds):
                        sem = opt_sem.at[half, k, group]
                        if out:
                            yield pltpu.make_async_copy(vmem.at[half, sub, q], hbm_out.at[layer, rows_, cols], sem)
                        else:
                            yield pltpu.make_async_copy(hbm.at[layer, rows_, cols], vmem.at[half, sub, q], sem)
                    if not out:
                        own = pl.ds(pl.multiple_of(me * r if wide else me * 8 * r + row, 8), r)
                        source = (wg_hbm, wu_hbm)[half] if wide else wd_hbm
                        yield pltpu.make_async_copy(source.at[layer, own, cols], wo.at[half, sub, q], opt_sem.at[half, 2, group])

        if not start:
            for half in range(2):
                for q in range(GROUPS):
                    for k, vmem in enumerate((mo, vo, wo)[: 2 if out else 3]):
                        block = (mg_hbm, vg_hbm, wg_hbm)[k].at[0, pl.ds(0, r), pl.ds(0, e)]
                        pltpu.make_async_copy(block, vmem.at[half, sub, q], opt_sem.at[half, k, sub * GROUPS + q]).wait()
            return
        for wide in (True, False):

            @pl.when(is_wide(piece) == wide)
            def _(wide=wide):
                for copy in copies(wide):
                    copy.start()

    def opt_step(piece, sub):
        for half in range(2):
            w, m, v = adamw(wo[half, sub].astype(F32), mo[half, sub], vo[half, sub], rs_sum(half, piece, sub))
            wn[half, sub], mo[half, sub], vo[half, sub] = w, m, v

    def go_on(event, piece, sub):
        if event < STAGES:
            if event >= 0:
                rs_wait(event, piece, sub)
            if 0 <= event < STAGES - 1:
                rs_add(event, piece, sub)
            if event < STAGES - 1:
                rs_start(event + 1, piece, sub)
            if event == STAGES - 2:
                opt_do(piece, sub, False, True)
            if event == STAGES - 1:
                opt_do(piece, sub, False, False)
                opt_step(piece, sub)
                opt_do(piece, sub, True, True)
                ag_start(0, piece, sub)
        else:
            ag_finish(event - STAGES, piece, sub)
            if event == STAGES:
                opt_do(piece, sub, True, False)
            if event < 2 * STAGES - 1:
                ag_start(event - STAGES + 1, piece, sub)

    def service(k, point):
        due = [(event - 1, sub, at) for sub in range(SUBS) for event, at in enumerate(TIMES[sub]) if at % POINTS == point]
        for event, sub, at in sorted(due, key=lambda one: (-one[0], -one[2], one[1])):
            piece = k - at // POINTS

            @pl.when(jnp.logical_and(piece >= 0, piece < PIECES))
            def _(event=event, piece=piece, sub=sub):
                go_on(event, piece, sub)

    def w_copy(which, layer, chunk):
        at_cols = pl.ds(pl.multiple_of(chunk * c, c), c)
        if which == 2:
            return pltpu.make_async_copy(wd_hbm.at[layer, at_cols, :], wd, w_sem.at[2])
        return pltpu.make_async_copy((wg_hbm, wu_hbm)[which].at[layer, :, at_cols], (wg, wu)[which], w_sem.at[which])

    def p_copy(piece, tile):
        slot = tile % 2
        at_cols = pl.ds(pl.multiple_of(chunk_of(piece) * c, c), c)
        return pltpu.make_async_copy(ps.at[slot], p1_hbm.at[pl.ds(pl.multiple_of(tile * rows, rows), rows), at_cols], p_sem.at[slot])

    def d_copy(which, chunk, tile, load):
        here = pl.ds(pl.multiple_of(tile * rows, rows), rows)
        vmem, hbm = (dg, du)[which].at[here, :], (dg_hbm, du_hbm)[which].at[chunk, here, :]
        return pltpu.make_async_copy(*((hbm, vmem) if load else (vmem, hbm)), d_sem.at[which, tile])

    def front_tile(piece, tile):
        here = pl.ds(pl.multiple_of(tile * rows, rows), rows)
        at_, dh_ = a[here, :], dh[here, :]

        @pl.when(tile >= 2)
        def _():
            p_copy(piece, tile - 2).wait()

        n = c // FRONT
        for j in range(FRONT):
            cols = slice(j * n, (j + 1) * n)
            gates, ups = dot(at_, wg[:, cols]), dot(at_, wu[:, cols])
            dps = dot(dh_, wd[cols, :], NT)
            for i in range(0, rows, STRIP):
                gate, up = gates[i : i + STRIP], ups[i : i + STRIP]
                dp = dps[i : i + STRIP].astype(BF).astype(F32)
                s = sigmoid(gate)
                gs = gate * s
                out = pl.ds(pl.multiple_of(tile * rows + i, STRIP), STRIP)
                ps[tile % 2, i : i + STRIP, cols] = (gs * up).astype(BF)
                du[out, cols] = (dp * gs).astype(BF)
                dg[out, cols] = (dp * up * (s + gs * (1.0 - s))).astype(BF)

        p_copy(piece, tile).start()
        for which in range(2):
            d_copy(which, chunk_of(piece), tile, False).start()

    def gu_copy(which, chunk, tile):
        slot = 2 * (tile % 2) + which
        source = (gate_hbm, up_hbm)[which].at[chunk, pl.ds(pl.multiple_of(tile * rows, rows), rows), :]
        return pltpu.make_async_copy(source, big.at[slot], gu_sem.at[slot])

    def kept_tile(piece, tile):
        here = pl.ds(pl.multiple_of(tile * rows, rows), rows)
        dh_ = dh[here, :]
        for which in range(2):
            gu_copy(which, chunk_of(piece), tile).wait()
        n = c // FRONT
        for j in range(FRONT):
            cols = slice(j * n, (j + 1) * n)
            dps = dot(dh_, wd[cols, :], NT)
            slot = 2 * (tile % 2)
            for i in range(0, rows, STRIP):
                gate, up = big[slot, i : i + STRIP, cols], big[slot + 1, i : i + STRIP, cols]
                dp = dps[i : i + STRIP].astype(BF).astype(F32)
                s = sigmoid(gate)
                gs = gate * s
                out = pl.ds(pl.multiple_of(tile * rows + i, STRIP), STRIP)
                du[out, cols] = (dp * gs).astype(BF)
                dg[out, cols] = (dp * up * (s + gs * (1.0 - s))).astype(BF)

        following = piece * tiles + tile + 2

        @pl.when(following < PIECES * tiles)
        def _():
            for which in range(2):
                gu_copy(which, following // tiles - CHUNKS - 2 * PARTS, following % tiles).start()

    def weight_part(side, which, piece):
        n = c // 2
        slot = piece % SLOTS
        term = dot(at[...], (dg, du)[which][:, pl.ds(pl.multiple_of(side * n, n), n)])
        for i in range(32):
            for q in range(2):
                group = side * 2 + q
                block = term[i * r : (i + 1) * r, q * e : (q + 1) * e].astype(BF)
                (ga, gb)[which][slot, group // GROUPS, place(i, ORDERS[which]), group % GROUPS] = block

    def through_layer(which, chunk, more):
        w_copy(which, 1, chunk).wait()

        def back(tile, _):
            here = pl.ds(pl.multiple_of(tile * rows, rows), rows)
            total = pl.ds(0, d)
            d_copy(which, chunk, tile, True).wait()
            part = dot((dg, du)[which][here, :], (wg, wu)[which][...], NT)
            if which == 0:
                big[tile, :, total] = jnp.where(chunk == 0, jnp.zeros_like(part), big[tile, :, total]) + part
            else:
                big[tile, :, total] += part

            @pl.when(more)
            def _():
                d_copy(which, chunk + 1, tile, True).start()

            return 0

        lax.fori_loop(0, tiles, back, 0)

        @pl.when(more)
        def _():
            w_copy(which, 1, chunk + 1).start()

    def tile_copy(which, tile, source):
        from_cols = pl.ds(pl.multiple_of(tile * wide, 128), wide)
        return pltpu.make_async_copy(source.at[:, from_cols], (dg, du)[which].at[:, pl.ds(0, wide)], load_sem.at[which])

    def tile_start(piece, which, tile):
        for layer, source in enumerate((p0_hbm, p1_hbm)):

            @pl.when(layer_of(piece) == layer)
            def _(source=source):
                tile_copy(which, tile, source).start()

    def down_all_tile(piece, which, tile):
        tile_copy(which, tile, p0_hbm).wait()
        places = [[place(4 * tile + i, order) for order in ORDERS] for i in range(4)]
        slots = [(piece + part) % SLOTS for part in range(PARTS)]
        for part in range(PARTS):
            term = dot(dht[part * e : (part + 1) * e, :], (dg, du)[which][:, :wide]).T
            for i in range(4):
                for j in range(8):
                    half, group = j // 4, j % 4
                    block = term[(8 * i + j) * r : (8 * i + j + 1) * r, :].astype(BF)
                    g_bufs[half][slots[part], group // GROUPS, places[i][half], group % GROUPS] = block

        @pl.when(tile + 2 < 8)
        def _():
            tile_start(piece, which, tile + 2)

    def down_tile(piece, which, tile):
        tile_copy(which, tile, p0_hbm).wait()
        at_rows = pl.ds(pl.multiple_of(part_of(piece) * e, e), e)
        places = [[place(4 * tile + i, order) for order in ORDERS] for i in range(4)]
        slot = piece % SLOTS
        term = dot(dht[at_rows, :], (dg, du)[which][:, :wide]).T
        for i in range(4):
            for j in range(8):
                half, group = j // 4, j % 4
                block = term[(8 * i + j) * r : (8 * i + j + 1) * r, :].astype(BF)
                g_bufs[half][slot, group // GROUPS, places[i][half], group % GROUPS] = block

        @pl.when(tile + 2 < 8)
        def _():
            tile_start(piece, which, tile + 2)

    def h_copy(tile):
        slot, here = tile % 2, pl.ds(pl.multiple_of(tile * rows, rows), rows)
        return pltpu.make_async_copy(h_hbm.at[here, :], ps.at[slot, :, pl.ds(0, d)], p_sem.at[slot])

    def through_norm():
        def back(tile, _):
            h_copy(tile).wait()

            def some(i, _):
                at_rows = pl.ds(pl.multiple_of(i * 32, 32), 32)
                at_all = pl.ds(pl.multiple_of(tile * rows + i * 32, 32), 32)
                h = ps[tile % 2, at_rows, pl.ds(0, d)].astype(F32)
                by_a = big[tile, at_rows, pl.ds(0, d)].astype(BF).astype(F32)
                scale = lax.rsqrt(jnp.mean(h * h, -1, keepdims=True) + 1e-6)
                along = jnp.sum(by_a * h, -1, keepdims=True)
                by_h = (by_a * scale - h * (scale * scale * scale * along * (1.0 / d))).astype(BF)
                dh[at_all, :] = (dh[at_all, :].astype(F32) + by_h.astype(F32)).astype(BF)
                return 0

            lax.fori_loop(0, rows // 32, some, 0)

            @pl.when(tile + 2 < tiles)
            def _():
                h_copy(tile + 2).start()

            return 0

        lax.fori_loop(0, tiles, back, 0)

    def turn(source, to):
        def back(tile, _):
            here = pl.ds(pl.multiple_of(tile * rows, rows), rows)
            to[:, here] = source[here, :].astype(F32).T.astype(BF)
            return 0

        lax.fori_loop(0, tiles, back, 0)

    def norm_all():
        def back(i, _):
            here = pl.ds(pl.multiple_of(i * 32, 32), 32)
            a[here, :] = normed(a[here, :])
            return 0

        lax.fori_loop(0, tokens // 32, back, 0)
        turn(a, at)

    first = (
        pltpu.make_async_copy(h_hbm, a, load_sem.at[2]),
        pltpu.make_async_copy(dy_hbm, dh, load_sem.at[3]),
        *(w_copy(which, 1, 0) for which in range(3)),
    )
    for copy in first:
        copy.start()
    first[0].wait()
    norm_all()
    first[1].wait()
    turn(dh, dht)
    x_copy = pltpu.make_async_copy(x_hbm, a, load_sem.at[2])

    def tick(k, _):
        computes = k < PIECES
        layer = layer_of(k)
        gated = jnp.logical_and(computes, is_wide(k))
        downs = jnp.logical_and(computes, jnp.logical_not(is_wide(k)))
        downs_0 = jnp.logical_and(downs, layer == 0)
        downs_1 = k == CHUNKS
        through = jnp.logical_and(k > CHUNKS, k < CHUNKS + PARTS)
        chunk = PARTS * (k - CHUNKS - 1)

        @pl.when(jnp.logical_or(downs_0, downs_1))
        def _():
            tile_start(k, 0, 0)
            tile_start(k, 1, 1)

        @pl.when(through)
        def _():
            for which in range(2):
                w_copy(which, 1, chunk).start()
                for tile in range(tiles):
                    d_copy(which, chunk, tile, True).start()

        def serve(point, points):
            for one in points:

                @pl.when(point == one)
                def _(one=one):
                    service(k, one)

        def fronts(point, _):
            serve(point, range(4))

            @pl.when(jnp.logical_and(gated, layer == 1))
            def _():
                @pl.when(point == 0)
                def _():
                    for which in range(3):
                        w_copy(which, 1, chunk_of(k)).wait()

                front_tile(k, point)

            @pl.when(jnp.logical_and(gated, layer == 0))
            def _():
                @pl.when(point == 0)
                def _():
                    w_copy(2, 0, chunk_of(k)).wait()

                kept_tile(k, point)

            @pl.when(downs_0)
            def _():
                for which in range(2):
                    down_tile(k, which, 2 * point + which)

            @pl.when(downs_1)
            def _():
                for which in range(2):
                    down_all_tile(k, which, 2 * point + which)

            for which in range(2):

                @pl.when(jnp.logical_and(through, point == 2 * which))
                def _(which=which):
                    through_layer(which, chunk, True)

            return 0

        lax.fori_loop(0, 4, fronts, 0)

        @pl.when(k < CHUNKS - 1)
        def _():
            for which in range(3):
                w_copy(which, 1, chunk_of(k) + 1).start()

        @pl.when(jnp.logical_and(k >= CHUNKS + 2 * PARTS, k < PIECES - 1))
        def _():
            w_copy(2, 0, chunk_of(k) + 1).start()

        def backs(side, _):
            for which in range(2):
                serve(4 + 2 * side + which, (4 + which, 6 + which))

                @pl.when(gated)
                def _(which=which):
                    weight_part(side, which, k)

                @pl.when(through)
                def _(which=which):
                    through_layer(which, chunk + 1 + side, side == 0)

            return 0

        lax.fori_loop(0, 2, backs, 0)

        @pl.when(jnp.logical_and(gated, layer == 1))
        def _():
            for tile in range(tiles - 2, tiles):
                p_copy(k, tile).wait()
            for which in range(2):
                for tile in range(tiles):
                    d_copy(which, chunk_of(k), tile, False).wait()

        @pl.when(k == CHUNKS - 1)
        def _():
            x_copy.start()
            for tile in range(2):
                h_copy(tile).start()

        @pl.when(k == CHUNKS + PARTS - 1)
        def _():
            w_copy(2, 0, 0).start()
            through_norm()
            for tile in range(2):
                for which in range(2):
                    gu_copy(which, 0, tile).start()
            turn(dh, dht)

        @pl.when(k == CHUNKS + PARTS)
        def _():
            x_copy.wait()
            norm_all()

        return 0

    lax.fori_loop(0, TICKS, tick, 0)


def train_step(x, dy, h, p0, gate, up, weights, ms, vs):
    tokens, d = dy.shape
    ff = p0.shape[1]
    c, r, e = ff // CHUNKS, d // 32, d // PARTS
    rows = min(512, tokens // 4)
    any_ = pl.BlockSpec(memory_space=pl.ANY)
    blocks = lambda *n: pltpu.VMEM((*n, GROUPS, r, e), BF)
    scratch = [
        pltpu.VMEM((tokens, d), BF), pltpu.VMEM((d, tokens), BF), pltpu.VMEM((tokens, d), BF), pltpu.VMEM((d, tokens), BF),
        pltpu.VMEM((d, c), BF), pltpu.VMEM((d, c), BF), pltpu.VMEM((c, d), BF),
        pltpu.VMEM((tokens, c), BF), pltpu.VMEM((tokens, c), BF),
        pltpu.VMEM((2, rows, c), BF),
        pltpu.VMEM((4, rows, c), F32),
        blocks(SLOTS, SUBS, 32), blocks(SLOTS, SUBS, 32),
        *[blocks(2, SUBS, 16 >> s) for s in range(STAGES)] * 2,
        *[blocks(SUBS, 16 >> s) for s in range(STAGES - 1)] * 2,
        blocks(2, SUBS), *[pltpu.VMEM((2, SUBS, GROUPS, r, e), F32)] * 2, blocks(2, SUBS),
        pltpu.SemaphoreType.DMA((2, STAGES, SUBS)), pltpu.SemaphoreType.DMA((2, STAGES, SUBS, 2)),
        pltpu.SemaphoreType.DMA((2, STAGES, SUBS)), pltpu.SemaphoreType.DMA((2, STAGES, SUBS, 2)),
        pltpu.SemaphoreType.DMA((2, SUBS)), pltpu.SemaphoreType.DMA((4,)), pltpu.SemaphoreType.DMA((3,)), pltpu.SemaphoreType.DMA((2,)),
        pltpu.SemaphoreType.DMA((2, 3, 4)), pltpu.SemaphoreType.DMA((2, 4)), pltpu.SemaphoreType.DMA((4,)),
    ]
    packed = jax.ShapeDtypeStruct((PIECES, SUBS, 32, GROUPS, r, e), BF)
    like = [jax.ShapeDtypeStruct(t.shape, F32) for t in (*ms, *vs)]
    return pl.pallas_call(
        step_kernel,
        name="step",
        in_specs=[any_] * 15,
        out_specs=[any_] * 11,
        out_shape=[packed, packed, *like, jax.ShapeDtypeStruct((tokens, ff), BF), *[jax.ShapeDtypeStruct((CHUNKS, tokens, c), BF)] * 2],
        scratch_shapes=scratch,
        compiler_params=pltpu.CompilerParams(collective_id=0, has_side_effects=True, vmem_limit_bytes=67_000_000),
        cost_estimate=pl.CostEstimate(flops=28 * tokens * d * ff, bytes_accessed=400 << 20, transcendentals=0),
    )(x, dy, h, p0, gate, up, *weights, *ms, *vs)


def unpack_kernel(gate_ref, up_ref, down_a, down_b, *refs):
    r, e = gate_ref.shape[-2:]
    moments, (wg_ref, wu_ref, wd_ref), moments_out = refs[:6], refs[6:9], refs[9:]
    for source, to in zip(moments, moments_out, strict=True):
        to[...] = source[...]
    for core in range(2):
        for z0 in range(2):
            for z1 in range(2):
                owner = z1 * 4 + z0 * 2 + core
                for group in range(4):
                    sub, q = group // GROUPS, group % GROUPS
                    for chunk in range(CHUNKS):
                        at_rows, at_cols = pl.ds(owner * r, r), pl.ds((chunk * 4 + group) * e, e)
                        wg_ref[at_rows, at_cols] = gate_ref[chunk, sub, core, z0, z1, q]
                        wu_ref[at_rows, at_cols] = up_ref[chunk, sub, core, z0, z1, q]
                    for part in range(PARTS):
                        for half, ref in enumerate((down_a, down_b)):
                            at_rows = pl.ds((owner * 8 + half * 4 + group) * r, r)
                            wd_ref[at_rows, pl.ds(part * e, e)] = ref[part, sub, core, z0, z1, q]


def unpack(wa, wb, moments, d, ff):
    r, e = wa.shape[-2:]
    wa, wb = (t.reshape(PIECES, SUBS, *(2,) * 5, GROUPS, r, e) for t in (wa, wb))

    def spec(n, first, half):
        def index(layer, x, y):
            outer, inner = (x, y) if half == 0 else (y, x)
            return (first(layer), 0, 0, outer, 0, inner, 0, 0, 0, 0)

        return pl.BlockSpec((n, SUBS, 2, None, 2, None, 2, GROUPS, r, e), index)

    wide, part = lambda layer: 2 - 2 * layer, lambda layer: 3 - layer
    slab = lambda rows, cols: pl.BlockSpec((None, rows, cols), lambda layer, x, y: (layer, 2 * x + y, 0))
    moment = [
        pl.BlockSpec((None, r, ff // 4), lambda layer, x, y: (layer, 0, 2 * x + y)) if t.shape[2] == ff else slab(2 * r, d) for t in moments
    ]
    return pl.pallas_call(
        unpack_kernel,
        name="unpack",
        grid=(2, 2, 2),
        in_specs=[spec(CHUNKS, wide, 0), spec(CHUNKS, wide, 1), spec(PARTS, part, 0), spec(PARTS, part, 1), *moment],
        out_specs=[slab(d // 4, ff), slab(d // 4, ff), slab(ff // 4, d), *moment],
        out_shape=[jax.ShapeDtypeStruct((2, d, ff), BF)] * 2
        + [jax.ShapeDtypeStruct((2, ff, d), BF)]
        + [jax.ShapeDtypeStruct(t.shape, F32) for t in moments],
        compiler_params=pltpu.CompilerParams(vmem_limit_bytes=60 << 20),
    )(wa, wb, wa, wb, *moments)


def solution(mesh):
    def step(x, dy, *arrays):
        wg, wu, wd = arrays[:3]
        ms, vs = arrays[3:6], arrays[6:9]
        x, dy = x[0], dy[0]
        p0, h, gate, up = forward(x, wg, wu, wd, 0)
        wa, wb, *moments, _, _, _ = train_step(x, dy, h, p0, gate, up, (wg, wu, wd), ms, vs)
        return tuple(unpack(wa, wb, moments, x.shape[1], wg.shape[2]))

    seq, whole, rows = P(("rep", "dp")), P(), P(None, "dp")
    return jax.shard_map(
        step,
        mesh=mesh,
        in_specs=(seq, seq) + (whole,) * 3 + (rows,) * 6,
        out_specs=(P("rep"),) * 3 + (P("rep", "dp"),) * 6,
        check_vma=False,
    )
```
